256 devices in a mesh: gx: 64 (over x, y_lo, z), gy: 4 (over y_hi, core).
Axes of the slice: x: 4, y: 4 (y_hi: 2, y_lo: 2; y = y_hi * 2 + y_lo), z: 8, core: 2. Of those that a mesh axis runs over, the one named last changes fastest.
Arguments:
- state: float32 [12, 4, 256, 8192], P(None, None, 'gy', 'gx'), may hold values from -240 to 240, as said below
- inverse: float32 [128, 256, 256], P('gy'), may hold values from -0.6 to 1.8, as said below
Outputs:
- updated: float32 [12, 4, 256, 8192], P(None, None, 'gy', 'gx')
- wall_stress: float32 [12, 2, 2, 8192], P(None, None, None, 'gx')
The draws below stay inside these ranges and needn't reach their ends.
Inputs may be any that keep to these rules, and one draw needn't show every extreme that they name: `state`: perturbation coefficients, of varying size over coefficients and x. Each inverse is a dense matrix with a positive diagonal.
All inputs are finite; a program needn't handle non-finite values.
Results may differ from the reference program's by a relative error of at most 0.0003.
Values sent between devices are 32-bit elements; how exact they have to be, the bound alone decides.
A program may use at most 64 MiB of HBM per device.

```python
import jax
import jax.numpy as jnp
from jax import lax

NY = 256
MODES = 128
X_DEV = 128
HALO = 64
MEMBERS = 12
NX = 8192
N_GX = 64


def draw_state(key, part):
    keys = jax.random.split(jax.random.fold_in(key, 11), 2)
    shape = (MEMBERS, 4, NY, NX)
    x_fraction = jnp.arange(NX, dtype=jnp.float32) / NX
    y_fraction = jnp.arange(NY, dtype=jnp.float32) / NY
    envelope = (1.0 + 2.0 * x_fraction)[None, None, None, :] * (1.0 + 2.0 * y_fraction)[None, None, :, None]
    roughness = jax.random.uniform(keys[1], shape, minval=0.5, maxval=1.5)
    base_draw = jnp.clip(jax.random.normal(keys[0], shape), -4.0, 4.0)
    return (base_draw * roughness * envelope).astype(jnp.float32)


def draw_inverse(key, part):
    keys = jax.random.split(jax.random.fold_in(key, 23), 2)
    diagonal = jnp.exp(jax.random.uniform(keys[0], (MODES, NY), minval=jnp.log(0.4), maxval=jnp.log(1.2)))
    identity = jnp.eye(NY, dtype=jnp.float32)
    noise = jnp.clip(jax.random.normal(keys[1], (MODES, NY, NY)), -5.0, 5.0) * 0.6 / jnp.sqrt(1.0 * NY)
    return (noise + identity[None, :, :] * diagonal[:, :, None]).astype(jnp.float32)


def setup_inputs(seed: int = 0) -> dict:
    key_list = jax.random.split(jax.random.key(seed), 3)
    state = draw_state(jax.random.fold_in(key_list[2], 71), 0)
    inverse = draw_inverse(jax.random.fold_in(key_list[2], 71), 0)
    return {"state": state, "inverse": inverse}


EPSILON = 1e-06
TIME_STEP = 0.5
MEAN_FLOW = 0.8
CORIOLIS = 0.6
STRATIFICATION = 0.9
HIGHEST = lax.Precision.HIGHEST

def window_tables(window, rim_width, points, mode_count):
    position = jnp.arange(window, dtype=jnp.int32)
    mode_index = jnp.arange(mode_count, dtype=jnp.int32)
    half_count = mode_count // 2
    is_cosine = mode_index <= half_count
    wave_index = jnp.where(is_cosine, mode_index, mode_index - half_count)
    product_index = position[:, None] * wave_index[None, :] % window
    phases = 2.0 * jnp.pi * product_index.astype(jnp.float32) / window
    wave_float = wave_index.astype(jnp.float32)
    weights_norm = jnp.where(wave_index == 0, jnp.sqrt(1.0 / window), jnp.sqrt(2.0 / window))
    fourier_basis = jnp.where(is_cosine[None, :], jnp.cos(phases), jnp.sin(phases)) * weights_norm[None, :]
    wavenumber = 2.0 * jnp.pi * wave_float / window
    paired = wave_index[:, None] == wave_index[None, :]
    to_sine = is_cosine[:, None] & jnp.logical_not(is_cosine[None, :]) & paired
    to_cosine = jnp.logical_not(is_cosine[:, None]) & is_cosine[None, :] & paired
    derivative = jnp.where(to_sine, -wavenumber[:, None], 0.0) + jnp.where(to_cosine, wavenumber[:, None], 0.0)
    position_float = position.astype(jnp.float32)
    window_taper = 0.25 + 0.75 * jnp.sin(jnp.pi * (position_float + 0.5) / window) ** 2
    slopes = jnp.dot(fourier_basis, derivative, precision=HIGHEST, preferred_element_type=jnp.float32)
    projection = jnp.concatenate([fourier_basis, slopes], axis=1) * window_taper[:, None]
    back_table = (fourier_basis[rim_width:rim_width + points, :] / window_taper[rim_width:rim_width + points, None]).T
    return (projection, back_table)

def advance(spectra, mode_count, coef_global, coef_count):
    modal_coef = spectra[..., :mode_count]
    slope = spectra[..., mode_count:]
    rhs_first = modal_coef[:, 0] + TIME_STEP * (-MEAN_FLOW * slope[:, 0] + CORIOLIS * modal_coef[:, 2])
    rhs_second = modal_coef[:, 1] + TIME_STEP * (-MEAN_FLOW * slope[:, 1] + modal_coef[:, 3])
    rhs_third = modal_coef[:, 2] + TIME_STEP * (-MEAN_FLOW * slope[:, 2] - CORIOLIS * modal_coef[:, 0])
    rhs_fourth = modal_coef[:, 3] + TIME_STEP * (-MEAN_FLOW * slope[:, 3] - STRATIFICATION * modal_coef[:, 1])
    stacked = jnp.stack([rhs_first, rhs_second, rhs_third, rhs_fourth], axis=1)
    interior = (coef_global < coef_count - 2)[None, None, :, None]
    return jnp.where(interior, stacked, 0.0)

def wall_weights(coef_global, coef_count):
    coef_float = coef_global.astype(jnp.float32)
    curvature = coef_float * coef_float / (coef_count * coef_count)
    parity = jnp.where(coef_global % 2 == 0, -1.0, 1.0)
    return jnp.stack([curvature, parity * curvature])

def reference(state, inverse):
    members, fields, coef_count, grid_x = state.shape
    window = X_DEV + 2 * HALO
    projection, back_table = window_tables(window, HALO, X_DEV, MODES)
    norm_sum = lax.optimization_barrier(jnp.sum(state * state, axis=(1, 2, 3)))
    renorm = lax.rsqrt(norm_sum / (fields * coef_count * grid_x) + EPSILON)
    padded = jnp.concatenate([state[..., grid_x - HALO:], state, state[..., :HALO]], axis=3)
    coef_global = jnp.arange(coef_count, dtype=jnp.int32)

    def one_window(window_index):
        segment = lax.dynamic_slice_in_dim(padded, (window_index * X_DEV).astype(jnp.int32), window, 3)
        spectra = jnp.dot(segment.reshape(-1, window), projection, precision=HIGHEST, preferred_element_type=jnp.float32)
        spectra = spectra.reshape(members, fields, coef_count, 2 * MODES)
        rhs = advance(spectra, MODES, coef_global, coef_count)
        solved = jnp.einsum('mij,efjm->efim', inverse, rhs, precision=HIGHEST)
        values = jnp.dot(solved.reshape(-1, MODES), back_table, precision=HIGHEST, preferred_element_type=jnp.float32)
        return values.reshape(members, fields, coef_count, X_DEV)
    pieces = lax.map(one_window, jnp.arange(N_GX, dtype=jnp.int32))
    updated = jnp.moveaxis(pieces, 0, 3).reshape(members, fields, coef_count, grid_x) * renorm[:, None, None, None]
    chosen = jnp.stack([updated[:, 0], updated[:, 2]], axis=1)
    wall_stress = jnp.einsum('wk,eckx->ewcx', wall_weights(coef_global, coef_count), chosen, precision=HIGHEST)
    return (updated, wall_stress)
```

```python
import functools

import jax
import jax.numpy as jnp
import numpy as np
from jax import lax
from jax.experimental import pallas as pl
from jax.experimental.pallas import tpu as pltpu
from jax.sharding import Mesh
from jax.sharding import PartitionSpec as P

MODES = 128
HALO = 64
AXES = ("gx_0", "gx_1", "gx_2", "gy_0", "gy_1")
GX = ("gx_0", "gx_1", "gx_2")
GY = ("gy_0", "gy_1")
EPSILON = 1e-06
TIME_STEP = 0.5
MEAN_FLOW = 0.8
CORIOLIS = 0.6
STRATIFICATION = 0.9
F32 = jnp.float32
BF16 = jnp.bfloat16
MESH = pl.DeviceIdType.MESH

MEMBERS = 12
FIELDS = 4
LOCAL = 64
PTS = 128
QUARTER = 32
BLOCK = 2 * QUARTER
STEP = 2
STEPS = MEMBERS // STEP
GROUP = 4
GROUPS = MEMBERS // GROUP
UNROLL = 8


def window_tables(window, rim, points, modes):
    pos = np.arange(window)
    mode = np.arange(modes)
    half = modes // 2
    cosine = mode <= half
    wave = np.where(cosine, mode, mode - half)
    phase = 2.0 * np.pi * (pos[:, None] * wave[None, :] % window) / window
    norm = np.where(wave == 0, np.sqrt(1.0 / window), np.sqrt(2.0 / window))
    basis = np.where(cosine[None, :], np.cos(phase), np.sin(phase)) * norm[None, :]
    kappa = 2.0 * np.pi * wave / window
    paired = wave[:, None] == wave[None, :]
    to_sine = cosine[:, None] & ~cosine[None, :] & paired
    to_cosine = ~cosine[:, None] & cosine[None, :] & paired
    derivative = np.where(to_sine, -kappa[:, None], 0.0) + np.where(to_cosine, kappa[:, None], 0.0)
    taper = 0.25 + 0.75 * np.sin(np.pi * (pos + 0.5) / window) ** 2
    plain = basis * taper[:, None]
    slope = (basis @ derivative) * taper[:, None]
    both = np.concatenate([plain - TIME_STEP * MEAN_FLOW * slope, plain], axis=1).T
    order = np.concatenate([np.arange(rim, window), np.arange(rim)])
    back = (basis[rim : rim + points] / taper[rim : rim + points, None]).T
    return both[:, order], back


def split_table(table):
    high = table.astype(BF16)
    low = (table - high.astype(np.float64)).astype(BF16)
    return high, low


def split(a):
    high = a.astype(BF16)
    low = (a - high.astype(F32)).astype(BF16)
    return high, low


def dot_t(a, b):
    return lax.dot_general(a, b, (((1,), (1,)), ((), ())), preferred_element_type=F32)


def dot(a, b):
    return lax.dot_general(a, b, (((1,), (0,)), ((), ())), preferred_element_type=F32)


def kernel(
    sizes,
    state_hbm, inverse_hbm, project_hbm, back_hbm, out_ref, wall_ref,
    state, inverse, inv_high, inv_low, project, back,
    to_right, to_left, from_left, from_right,
    out_modes, in_modes, out_coefs, in_coefs,
    sum_mine, sum_theirs, wall_mine, wall_all,
    local_sem, halo_send, halo_recv, mode_send, mode_recv, coef_send, coef_recv,
    sum_send, sum_recv, wall_send, wall_recv,
):
    nx, ny, nz = sizes
    x, y, z = (lax.axis_index(a) for a in GX)
    hi, core = (lax.axis_index(a) for a in GY)
    me = hi * 2 + core
    count = nx * ny * nz
    here = (x * ny + y) * nz + z

    def place(index):
        return {
            "gx_0": lax.div(index, ny * nz),
            "gx_1": lax.rem(lax.div(index, nz), ny),
            "gx_2": lax.rem(index, nz),
        }

    right = place(lax.rem(here + 1, count))
    left = place(lax.rem(here + count - 1, count))
    solvers = [{"gx_1": 1 - y, "gy_0": q // 2, "gy_1": q % 2} for q in range(4)]

    def other(step):
        index = lax.rem(me + step, 4)
        return index, {"gy_0": lax.div(index, 2), "gy_1": lax.rem(index, 2)}

    partners = [{"gy_1": 1 - core}, {"gx_1": 1 - y}, {"gy_0": 1 - hi}]
    for name, value, size in (("gx_0", x, nx), ("gx_2", z, nz)):
        bit = 1
        while bit < size:
            flip = value + bit - 2 * bit * lax.rem(lax.div(value, bit), 2)
            partners.append({name: flip})
            bit *= 2
    rounds = len(partners)

    barrier = pltpu.get_barrier_semaphore()
    met = [right, left, *solvers, other(1)[1], other(2)[1], other(3)[1], *partners[3:]]
    for device in met:
        pl.semaphore_signal(barrier, inc=1, device_id=device, device_id_type=MESH)

    loads = [
        pltpu.make_async_copy(state_hbm, state, local_sem.at[0]),
        pltpu.make_async_copy(project_hbm, project, local_sem.at[1]),
        pltpu.make_async_copy(back_hbm, back, local_sem.at[2]),
    ]
    for k in range(4):
        part = pl.ds(k * 8, 8)
        loads.append(
            pltpu.make_async_copy(inverse_hbm.at[part], inverse.at[part], local_sem.at[3 + k])
        )
    for load in loads:
        load.start()

    lane = lax.broadcasted_iota(jnp.int32, (1, PTS), 1)
    low_half = lane < LOCAL

    def halo_copies(step):
        rows = pl.ds(step * STEP, STEP)
        return (
            pltpu.make_async_remote_copy(
                to_right.at[rows], from_left.at[rows], halo_send.at[0, step], halo_recv.at[0, step],
                device_id=right, device_id_type=MESH,
            ),
            pltpu.make_async_remote_copy(
                to_left.at[rows], from_right.at[rows], halo_send.at[1, step], halo_recv.at[1, step],
                device_id=left, device_id_type=MESH,
            ),
        )

    loads[0].wait()

    def pack(e):
        centre = state[e]
        top, low = centre[:, :32], centre[:, 32:]
        turned = pltpu.roll(low, LOCAL, 2)
        to_right[e] = jnp.where(low_half, turned, top)
        to_left[e] = jnp.where(low_half, top, turned)

    pack(0)
    pack(1)
    pl.semaphore_wait(barrier, len(met))
    for copy in halo_copies(0):
        copy.start()

    def pack_and_send(step, carry):
        pack(step * STEP)
        pack(step * STEP + 1)
        for copy in halo_copies(step):
            copy.start()
        return carry

    lax.fori_loop(1, STEPS, pack_and_send, 0)

    sum_mine[0] = jnp.zeros((16, PTS), F32)

    def squares(e, carry):
        values = state[e].reshape(FIELDS * LOCAL, PTS)
        sum_mine[0, pl.ds(e, 1), :] = jnp.sum(values * values, axis=0, keepdims=True)
        return carry

    lax.fori_loop(0, MEMBERS, squares, 0)

    def sum_copy(k):
        return pltpu.make_async_remote_copy(
            sum_mine.at[k], sum_theirs.at[k], sum_send.at[k], sum_recv.at[k],
            device_id=partners[k], device_id_type=MESH,
        )

    sum_copy(0).start()

    def sum_round(k):
        sum_copy(k).wait_recv()
        sum_mine[k + 1] = sum_mine[k] + sum_theirs[k]
        if k + 1 < rounds:
            sum_copy(k + 1).start()

    for load in loads[1:]:
        load.wait()

    def split_inverse(m, carry):
        high, low = split(inverse[m])
        inv_high[m] = high
        inv_low[m] = low
        return carry

    lax.fori_loop(0, QUARTER, split_inverse, 0)

    coupling_0 = jnp.where(low_half, TIME_STEP * CORIOLIS, TIME_STEP)
    coupling_1 = jnp.where(low_half, -TIME_STEP * CORIOLIS, -TIME_STEP * STRATIFICATION)
    coefficient = me * LOCAL + lax.rem(lane, LOCAL)
    interior = coefficient < 4 * LOCAL - 2

    def mode_copies(step):
        rows = pl.ds(step * (STEP * BLOCK), STEP * BLOCK)
        return [
            pltpu.make_async_remote_copy(
                out_modes.at[q, rows], in_modes.at[me, rows],
                mode_send.at[q, step], mode_recv.at[me, step],
                device_id=solvers[q], device_id_type=MESH,
            )
            for q in range(4)
        ]

    def project_member(e):
        centre = state[e]
        rim_left, rim_right = from_left[e], from_right[e]
        top = jnp.where(low_half, rim_right, rim_left)
        low = pltpu.roll(jnp.where(low_half, rim_left, rim_right), LOCAL, 2)
        rim = jnp.concatenate([top, low], axis=1)
        segment = jnp.concatenate(
            [centre.reshape(FIELDS * LOCAL, PTS), rim.reshape(FIELDS * LOCAL, PTS)], axis=1
        )
        high, low = split(segment)
        first = dot_t(project[...], high)
        second = dot_t(project[: 2 * MODES], low)
        both = first[: 2 * MODES] + (first[2 * MODES :] + second)
        a_0, a_1 = both[:MODES, :PTS], both[:MODES, PTS:]
        b_0, b_1 = both[MODES:, :PTS], both[MODES:, PTS:]
        rhs_0 = jnp.where(interior, a_0 + coupling_0 * b_1, 0.0)
        rhs_1 = jnp.where(interior, a_1 + coupling_1 * b_0, 0.0)
        for q in range(4):
            modes = slice(q * QUARTER, (q + 1) * QUARTER)
            base = pl.multiple_of(e * BLOCK, BLOCK)
            out_modes[q, pl.ds(base, QUARTER), :] = rhs_0[modes]
            out_modes[q, pl.ds(base + QUARTER, QUARTER), :] = rhs_1[modes]

    def project_step(step, carry):
        for copy in halo_copies(step):
            copy.wait_recv()
        for k in range(STEP):
            project_member(step * STEP + k)
        for copy in mode_copies(step):
            copy.start()
        for k in range(min(rounds, STEPS)):
            @pl.when(step == k)
            def _():
                sum_round(k)
        return carry

    lax.fori_loop(0, STEPS, project_step, 0)
    for k in range(STEPS, rounds):
        sum_round(k)

    def coef_copies(group):
        rows = pl.ds(group * (GROUP * BLOCK), GROUP * BLOCK)
        return [
            pltpu.make_async_remote_copy(
                out_coefs.at[t, rows], in_coefs.at[me, rows],
                coef_send.at[t, group], coef_recv.at[me, group],
                device_id=solvers[t], device_id_type=MESH,
            )
            for t in range(4)
        ]

    def arrived(buffer, sem, rows, s, k):
        return pltpu.make_async_remote_copy(
            buffer.at[s, rows], buffer.at[s, rows], sem.at[s, k], sem.at[s, k],
            device_id=solvers[s], device_id_type=MESH,
        )

    def turn(a):
        return pltpu.roll(a, LOCAL, 1)

    def solve_mode(base, m):
        rows = pl.ds(base + m, 2 * GROUP, stride=QUARTER)
        parts = [in_modes[s, rows, :] for s in range(4)]
        even, odd = [], []
        for s in (0, 2):
            first, second = parts[s], parts[s + 1]
            even.append(jnp.where(low_half, first, turn(second)))
            odd.append(jnp.where(low_half, turn(first), second))
        values = jnp.concatenate(
            [jnp.concatenate(even, axis=1), jnp.concatenate(odd, axis=1)], axis=0
        )
        high, low = split(values)
        count = 4 * GROUP
        first = dot_t(jnp.concatenate([high, low], axis=0), inv_high[m])
        second = dot_t(high, inv_low[m])
        solved = first[:count] + (first[count:] + second)
        even, odd = solved[: 2 * GROUP], solved[2 * GROUP :]
        for k in range(2):
            lanes = slice(k * PTS, (k + 1) * PTS)
            out_coefs[2 * k, rows, :] = jnp.where(low_half, even[:, lanes], turn(odd[:, lanes]))
            out_coefs[2 * k + 1, rows, :] = jnp.where(low_half, turn(even[:, lanes]), odd[:, lanes])

    def solve_group(group, carry):
        for s in range(4):
            for k in range(GROUP // STEP):
                step = group * (GROUP // STEP) + k
                rows = pl.ds(step * (STEP * BLOCK), STEP * BLOCK)
                arrived(in_modes, mode_recv, rows, s, step).wait_recv()
        base = group * (GROUP * BLOCK)

        def some_modes(k, carry):
            for u in range(UNROLL):
                solve_mode(base, k * UNROLL + u)
            return carry

        lax.fori_loop(0, QUARTER // UNROLL, some_modes, 0)
        for copy in coef_copies(group):
            copy.start()
        return carry

    lax.fori_loop(0, GROUPS, solve_group, 0)

    row = lax.broadcasted_iota(jnp.int32, (LOCAL, PTS), 0)
    k_float = (me * LOCAL + row).astype(F32)
    curvature = k_float * k_float / float((4 * LOCAL) ** 2)
    parity = jnp.where(lax.rem(row[:8], 2) == 0, -1.0, 1.0)
    grid = float(FIELDS * 4 * LOCAL * PTS * count)

    def back_member(e):
        base = pl.multiple_of(e * BLOCK, BLOCK)
        turned = []
        for col in range(2):
            block = jnp.concatenate(
                [in_coefs[q, pl.ds(base + col * QUARTER, QUARTER), :] for q in range(4)], axis=0
            )
            turned.append(block.T)
        high, low = split(jnp.concatenate(turned, axis=0))
        values = dot(jnp.concatenate([high, low], axis=1), back[: 2 * MODES])
        values = values + dot(high, back[2 * MODES :])
        total = jnp.sum(sum_mine[rounds, pl.ds(e, 1), :], axis=1, keepdims=True)
        values = values * lax.rsqrt(total / grid + EPSILON)
        out_ref[e] = values.reshape(FIELDS, LOCAL, PTS)
        for c in range(2):
            weighted = values[c * PTS : c * PTS + LOCAL] * curvature
            rows = jnp.sum(weighted.reshape(LOCAL // 8, 8, PTS), axis=0)
            wall_mine[pl.ds(e * 4 + c, 1), :] = jnp.sum(rows, axis=0, keepdims=True)
            wall_mine[pl.ds(e * 4 + 2 + c, 1), :] = jnp.sum(rows * parity, axis=0, keepdims=True)

    def back_group(group, carry):
        rows = pl.ds(group * (GROUP * BLOCK), GROUP * BLOCK)
        for s in range(4):
            arrived(in_coefs, coef_recv, rows, s, group).wait_recv()

        def one(k, carry):
            back_member(group * GROUP + k)
            return carry

        lax.fori_loop(0, GROUP, one, 0)
        return carry

    lax.fori_loop(0, GROUPS, back_group, 0)

    def wall_copy(step):
        index, device = other(step)
        send = pltpu.make_async_remote_copy(
            wall_mine, wall_all.at[me], wall_send.at[step - 1], wall_recv.at[me],
            device_id=device, device_id_type=MESH,
        )
        receive = pltpu.make_async_remote_copy(
            wall_mine, wall_all.at[index], wall_send.at[step - 1], wall_recv.at[index],
            device_id=device, device_id_type=MESH,
        )
        return send, receive

    for step in (1, 2, 3):
        wall_copy(step)[0].start()
    wall_all[me] = wall_mine[...]

    def ended(step, carry):
        for copy in halo_copies(step):
            copy.wait_send()
        for copy in mode_copies(step):
            copy.wait_send()
        return carry

    lax.fori_loop(0, STEPS, ended, 0)

    def ended_group(group, carry):
        for copy in coef_copies(group):
            copy.wait_send()
        return carry

    lax.fori_loop(0, GROUPS, ended_group, 0)
    for k in range(rounds):
        sum_copy(k).wait_send()
    for step in (1, 2, 3):
        wall_copy(step)[0].wait_send()
        wall_copy(step)[1].wait_recv()
    wall_ref[...] = (wall_all[0] + wall_all[1]) + (wall_all[2] + wall_all[3])


def per_device(sizes, state, inverse):
    both, back = window_tables(PTS + 2 * HALO, HALO, PTS, MODES)
    project = jnp.asarray(np.concatenate(split_table(both), axis=0))
    high, low = split_table(back)
    back = jnp.asarray(np.concatenate([high, high, low], axis=0))
    rounds = 3 + (sizes[0].bit_length() - 1) + (sizes[2].bit_length() - 1)
    exchange = (4, MEMBERS * BLOCK, PTS)
    rim = (MEMBERS, FIELDS, 32, PTS)
    vmem = pltpu.VMEM
    dma = pltpu.SemaphoreType.DMA
    updated, wall = pl.pallas_call(
        functools.partial(kernel, sizes),
        out_shape=(
            jax.ShapeDtypeStruct(state.shape, F32),
            jax.ShapeDtypeStruct((4 * MEMBERS, PTS), F32),
        ),
        in_specs=[pl.BlockSpec(memory_space=pl.ANY)] * 4,
        out_specs=(
            pl.BlockSpec(memory_space=pltpu.VMEM),
            pl.BlockSpec(memory_space=pltpu.VMEM),
        ),
        scratch_shapes=[
            vmem(state.shape, F32),
            vmem(inverse.shape, F32),
            vmem(inverse.shape, BF16),
            vmem(inverse.shape, BF16),
            vmem(project.shape, BF16),
            vmem(back.shape, BF16),
            *[vmem(rim, F32)] * 4,
            *[vmem(exchange, F32)] * 4,
            vmem((rounds + 1, 16, PTS), F32),
            vmem((rounds, 16, PTS), F32),
            vmem((4 * MEMBERS, PTS), F32),
            vmem((4, 4 * MEMBERS, PTS), F32),
            dma((7,)),
            dma((2, STEPS)),
            dma((2, STEPS)),
            dma((4, STEPS)),
            dma((4, STEPS)),
            dma((4, GROUPS)),
            dma((4, GROUPS)),
            dma((rounds,)),
            dma((rounds,)),
            dma((3,)),
            dma((4,)),
        ],
        compiler_params=pltpu.CompilerParams(
            collective_id=0, has_side_effects=True, vmem_limit_bytes=56 * 1024 * 1024
        ),
        name="step",
    )(state, inverse, project, back)
    return updated, wall.reshape(MEMBERS, 2, 2, PTS)


def solution(mesh):
    torus = Mesh(mesh.devices.reshape(4, 2, 8, 2, 2), AXES)
    return jax.shard_map(
        functools.partial(per_device, (4, 2, 8)),
        mesh=torus,
        in_specs=(P(None, None, GY, GX), P(GY, None, None)),
        out_specs=(P(None, None, GY, GX), P(None, None, None, GX)),
        check_vma=False,
    )
```

```python
import functools

import jax
import jax.numpy as jnp
import numpy as np
from jax import lax
from jax.experimental import pallas as pl
from jax.experimental.pallas import tpu as pltpu
from jax.sharding import Mesh
from jax.sharding import PartitionSpec as P

MODES = 128
HALO = 64
AXES = ("gx_0", "gx_1", "gx_2", "gy_0", "gy_1")
GX = ("gx_0", "gx_1", "gx_2")
GY = ("gy_0", "gy_1")
EPSILON = 1e-06
TIME_STEP = 0.5
MEAN_FLOW = 0.8
CORIOLIS = 0.6
STRATIFICATION = 0.9
F32 = jnp.float32
BF16 = jnp.bfloat16
MESH = pl.DeviceIdType.MESH

MEMBERS = 12
FIELDS = 4
LOCAL = 64
PTS = 128
QUARTER = 32
BLOCK = 2 * QUARTER
STEP = 2
STEPS = MEMBERS // STEP
GROUP = 4
GROUPS = MEMBERS // GROUP
UNROLL = 8


def window_tables(window, rim, points, modes):
    pos = np.arange(window)
    mode = np.arange(modes)
    half = modes // 2
    cosine = mode <= half
    wave = np.where(cosine, mode, mode - half)
    phase = 2.0 * np.pi * (pos[:, None] * wave[None, :] % window) / window
    norm = np.where(wave == 0, np.sqrt(1.0 / window), np.sqrt(2.0 / window))
    basis = np.where(cosine[None, :], np.cos(phase), np.sin(phase)) * norm[None, :]
    kappa = 2.0 * np.pi * wave / window
    paired = wave[:, None] == wave[None, :]
    to_sine = cosine[:, None] & ~cosine[None, :] & paired
    to_cosine = ~cosine[:, None] & cosine[None, :] & paired
    derivative = np.where(to_sine, -kappa[:, None], 0.0) + np.where(to_cosine, kappa[:, None], 0.0)
    taper = 0.25 + 0.75 * np.sin(np.pi * (pos + 0.5) / window) ** 2
    plain = basis * taper[:, None]
    slope = (basis @ derivative) * taper[:, None]
    both = np.concatenate([plain - TIME_STEP * MEAN_FLOW * slope, plain], axis=1).T
    order = np.concatenate([np.arange(rim, window), np.arange(rim)])
    back = (basis[rim : rim + points] / taper[rim : rim + points, None]).T
    return both[:, order], back


def split_table(table):
    high = table.astype(BF16)
    low = (table - high.astype(np.float64)).astype(BF16)
    return high, low


def split(a):
    high = a.astype(BF16)
    low = (a - high.astype(F32)).astype(BF16)
    return high, low


def dot_t(a, b):
    return lax.dot_general(a, b, (((1,), (1,)), ((), ())), preferred_element_type=F32)


def dot(a, b):
    return lax.dot_general(a, b, (((1,), (0,)), ((), ())), preferred_element_type=F32)


def kernel(
    sizes,
    state_hbm, inverse_hbm, project_hbm, back_hbm, out_ref, wall_ref,
    state, inverse, inv_high, inv_low, project, back,
    to_right, to_left, from_left, from_right,
    out_modes, in_modes, out_coefs, in_coefs,
    sum_mine, sum_all, wall_mine, wall_all,
    local_sem, halo_send, halo_recv, mode_send, mode_recv, coef_send, coef_recv,
    sum_send, sum_recv, wall_send, wall_recv,
):
    nx, ny, nz = sizes
    x, y, z = (lax.axis_index(a) for a in GX)
    hi, core = (lax.axis_index(a) for a in GY)
    me = hi * 2 + core
    count = nx * ny * nz
    here = (x * ny + y) * nz + z

    def place(index):
        return {
            "gx_0": lax.div(index, ny * nz),
            "gx_1": lax.rem(lax.div(index, nz), ny),
            "gx_2": lax.rem(index, nz),
        }

    right = place(lax.rem(here + 1, count))
    left = place(lax.rem(here + count - 1, count))
    solvers = [{"gx_1": 1 - y, "gy_0": q // 2, "gy_1": q % 2} for q in range(4)]

    def other(step):
        index = lax.rem(me + step, 4)
        return index, {"gy_0": lax.div(index, 2), "gy_1": lax.rem(index, 2)}

    def stage_peer(stage, step):
        if stage == 0:
            index = lax.rem(z + step, nz)
            return index, {"gx_2": index}
        if stage == 1:
            index = lax.rem(x + step, nx)
            return index, {"gx_0": index}
        index = lax.rem(y * 4 + me + step, 4 * ny)
        return index, {
            "gx_1": lax.div(index, 4),
            "gy_0": lax.rem(lax.div(index, 2), 2),
            "gy_1": lax.rem(index, 2),
        }

    stage_me = (z, x, y * 4 + me)
    stage_size = (nz, nx, 4 * ny)
    peers = [stage_peer(k, n)[1] for k in range(3) for n in range(1, stage_size[k])]

    barrier = pltpu.get_barrier_semaphore()
    met = [right, left, *peers]
    for device in met:
        pl.semaphore_signal(barrier, inc=1, device_id=device, device_id_type=MESH)

    state_load = pltpu.make_async_copy(state_hbm, state, local_sem.at[0])
    state_load.start()
    loads = [
        pltpu.make_async_copy(project_hbm, project, local_sem.at[1]),
        pltpu.make_async_copy(back_hbm, back, local_sem.at[2]),
    ]
    for k in range(4):
        part = pl.ds(k * 8, 8)
        loads.append(
            pltpu.make_async_copy(inverse_hbm.at[part], inverse.at[part], local_sem.at[3 + k])
        )

    lane = lax.broadcasted_iota(jnp.int32, (1, PTS), 1)
    low_half = lane < LOCAL

    def halo_copies(step):
        rows = pl.ds(step * STEP, STEP)
        return (
            pltpu.make_async_remote_copy(
                to_right.at[rows], from_left.at[rows], halo_send.at[0, step], halo_recv.at[0, step],
                device_id=right, device_id_type=MESH,
            ),
            pltpu.make_async_remote_copy(
                to_left.at[rows], from_right.at[rows], halo_send.at[1, step], halo_recv.at[1, step],
                device_id=left, device_id_type=MESH,
            ),
        )

    state_load.wait()
    for load in loads:
        load.start()

    def pack(e):
        centre = state[e]
        top, low = centre[:, :32], centre[:, 32:]
        turned = pltpu.roll(low, LOCAL, 2)
        to_right[e] = jnp.where(low_half, turned, top)
        to_left[e] = jnp.where(low_half, top, turned)

    for k in range(STEP):
        pack(k)

    def squares(e, carry):
        values = state[e].reshape(FIELDS * LOCAL, PTS)
        total = jnp.sum(values * values, axis=0, keepdims=True)
        return jnp.where(lane == e, jnp.sum(total, axis=1, keepdims=True), carry)

    sum_mine[0] = lax.fori_loop(0, MEMBERS, squares, jnp.zeros((1, PTS), F32))

    def sum_copies(stage, step):
        index, device = stage_peer(stage, step)

        def copy(slot):
            return pltpu.make_async_remote_copy(
                sum_mine.at[stage], sum_all.at[stage, slot],
                sum_send.at[stage, step - 1], sum_recv.at[stage, slot],
                device_id=device, device_id_type=MESH,
            )

        return copy(stage_me[stage]), copy(index)

    def sum_start(stage):
        for step in range(1, stage_size[stage]):
            sum_copies(stage, step)[0].start()
        sum_all[stage, stage_me[stage]] = sum_mine[stage]

    def sum_end(stage):
        for step in range(1, stage_size[stage]):
            sum_copies(stage, step)[1].wait_recv()
        total = sum_all[stage, 0]
        for k in range(1, stage_size[stage]):
            total = total + sum_all[stage, k]
        sum_mine[stage + 1] = total

    pl.semaphore_wait(barrier, len(met))
    sum_start(0)
    for copy in halo_copies(0):
        copy.start()

    def pack_and_send(step, carry):
        for k in range(STEP):
            pack(step * STEP + k)
        for copy in halo_copies(step):
            copy.start()
        return carry

    lax.fori_loop(1, STEPS, pack_and_send, 0)

    for load in loads:
        load.wait()

    def split_inverse(m, carry):
        high, low = split(inverse[m])
        inv_high[m] = high
        inv_low[m] = low
        return carry

    lax.fori_loop(0, QUARTER, split_inverse, 0)

    coupling_0 = jnp.where(low_half, TIME_STEP * CORIOLIS, TIME_STEP)
    coupling_1 = jnp.where(low_half, -TIME_STEP * CORIOLIS, -TIME_STEP * STRATIFICATION)
    coefficient = me * LOCAL + lax.rem(lane, LOCAL)
    interior = coefficient < 4 * LOCAL - 2

    def mode_copies(step):
        rows = pl.ds(step * (STEP * BLOCK), STEP * BLOCK)
        return [
            pltpu.make_async_remote_copy(
                out_modes.at[q, rows], in_modes.at[me, rows],
                mode_send.at[q, step], mode_recv.at[me, step],
                device_id=solvers[q], device_id_type=MESH,
            )
            for q in range(4)
        ]

    def project_member(e):
        centre = state[e]
        rim_left, rim_right = from_left[e], from_right[e]
        top = jnp.where(low_half, rim_right, rim_left)
        low = pltpu.roll(jnp.where(low_half, rim_left, rim_right), LOCAL, 2)
        rim = jnp.concatenate([top, low], axis=1)
        segment = jnp.concatenate(
            [centre.reshape(FIELDS * LOCAL, PTS), rim.reshape(FIELDS * LOCAL, PTS)], axis=1
        )
        high, low = split(segment)
        first = dot_t(project[...], high)
        second = dot_t(project[: 2 * MODES], low)
        both = first[: 2 * MODES] + (first[2 * MODES :] + second)
        a_0, a_1 = both[:MODES, :PTS], both[:MODES, PTS:]
        b_0, b_1 = both[MODES:, :PTS], both[MODES:, PTS:]
        rhs_0 = jnp.where(interior, a_0 + coupling_0 * b_1, 0.0)
        rhs_1 = jnp.where(interior, a_1 + coupling_1 * b_0, 0.0)
        for q in range(4):
            modes = slice(q * QUARTER, (q + 1) * QUARTER)
            base = pl.multiple_of(e * BLOCK, BLOCK)
            out_modes[q, pl.ds(base, QUARTER), :] = rhs_0[modes]
            out_modes[q, pl.ds(base + QUARTER, QUARTER), :] = rhs_1[modes]

    def project_step(step, carry):
        for copy in halo_copies(step):
            copy.wait_recv()
        for k in range(STEP):
            project_member(step * STEP + k)
        for copy in mode_copies(step):
            copy.start()

        @pl.when(step == 2)
        def _():
            sum_end(0)
            sum_start(1)

        @pl.when(step == 4)
        def _():
            sum_end(1)
            sum_start(2)

        return carry

    lax.fori_loop(0, STEPS, project_step, 0)

    def coef_copies(group):
        rows = pl.ds(group * (GROUP * BLOCK), GROUP * BLOCK)
        return [
            pltpu.make_async_remote_copy(
                out_coefs.at[t, rows], in_coefs.at[me, rows],
                coef_send.at[t, group], coef_recv.at[me, group],
                device_id=solvers[t], device_id_type=MESH,
            )
            for t in range(4)
        ]

    def arrived(buffer, sem, rows, s, k):
        return pltpu.make_async_remote_copy(
            buffer.at[s, rows], buffer.at[s, rows], sem.at[s, k], sem.at[s, k],
            device_id=solvers[s], device_id_type=MESH,
        )

    def turn(a):
        return pltpu.roll(a, LOCAL, 1)

    def solve_mode(base, m):
        rows = pl.ds(base + m, 2 * GROUP, stride=QUARTER)
        parts = [in_modes[s, rows, :] for s in range(4)]
        even, odd = [], []
        for s in (0, 2):
            first, second = parts[s], parts[s + 1]
            even.append(jnp.where(low_half, first, turn(second)))
            odd.append(jnp.where(low_half, turn(first), second))
        values = jnp.concatenate(
            [jnp.concatenate(even, axis=1), jnp.concatenate(odd, axis=1)], axis=0
        )
        high, low = split(values)
        count = 4 * GROUP
        first = dot_t(jnp.concatenate([high, low], axis=0), inv_high[m])
        second = dot_t(high, inv_low[m])
        solved = first[:count] + (first[count:] + second)
        even, odd = solved[: 2 * GROUP], solved[2 * GROUP :]
        for k in range(2):
            lanes = slice(k * PTS, (k + 1) * PTS)
            out_coefs[2 * k, rows, :] = jnp.where(low_half, even[:, lanes], turn(odd[:, lanes]))
            out_coefs[2 * k + 1, rows, :] = jnp.where(low_half, turn(even[:, lanes]), odd[:, lanes])

    def solve_group(group, carry):
        for s in range(4):
            for k in range(GROUP // STEP):
                step = group * (GROUP // STEP) + k
                rows = pl.ds(step * (STEP * BLOCK), STEP * BLOCK)
                arrived(in_modes, mode_recv, rows, s, step).wait_recv()
        base = group * (GROUP * BLOCK)

        def some_modes(k, carry):
            for u in range(UNROLL):
                solve_mode(base, k * UNROLL + u)
            return carry

        lax.fori_loop(0, QUARTER // UNROLL, some_modes, 0)
        for copy in coef_copies(group):
            copy.start()
        return carry

    lax.fori_loop(0, GROUPS, solve_group, 0)

    row = lax.broadcasted_iota(jnp.int32, (LOCAL, PTS), 0)
    k_float = (me * LOCAL + row).astype(F32)
    curvature = k_float * k_float / float((4 * LOCAL) ** 2)
    parity = jnp.where(lax.rem(row[:8], 2) == 0, -1.0, 1.0)
    grid = float(FIELDS * 4 * LOCAL * PTS * count)

    sum_end(2)

    def back_member(e):
        base = pl.multiple_of(e * BLOCK, BLOCK)
        turned = []
        for col in range(2):
            block = jnp.concatenate(
                [in_coefs[q, pl.ds(base + col * QUARTER, QUARTER), :] for q in range(4)], axis=0
            )
            turned.append(block.T)
        high, low = split(jnp.concatenate(turned, axis=0))
        values = dot(jnp.concatenate([high, low], axis=1), back[: 2 * MODES])
        values = values + dot(high, back[2 * MODES :])
        total = jnp.sum(jnp.where(lane == e, sum_mine[3], 0.0), axis=1, keepdims=True)
        values = values * lax.rsqrt(total / grid + EPSILON)
        out_ref[e] = values.reshape(FIELDS, LOCAL, PTS)
        for c in range(2):
            weighted = values[c * PTS : c * PTS + LOCAL] * curvature
            rows = jnp.sum(weighted.reshape(LOCAL // 8, 8, PTS), axis=0)
            wall_mine[pl.ds(e * 4 + c, 1), :] = jnp.sum(rows, axis=0, keepdims=True)
            wall_mine[pl.ds(e * 4 + 2 + c, 1), :] = jnp.sum(rows * parity, axis=0, keepdims=True)

    def back_group(group, carry):
        rows = pl.ds(group * (GROUP * BLOCK), GROUP * BLOCK)
        for s in range(4):
            arrived(in_coefs, coef_recv, rows, s, group).wait_recv()

        def one(k, carry):
            back_member(group * GROUP + k)
            return carry

        lax.fori_loop(0, GROUP, one, 0)
        return carry

    lax.fori_loop(0, GROUPS, back_group, 0)

    def wall_copy(step):
        index, device = other(step)
        send = pltpu.make_async_remote_copy(
            wall_mine, wall_all.at[me], wall_send.at[step - 1], wall_recv.at[me],
            device_id=device, device_id_type=MESH,
        )
        receive = pltpu.make_async_remote_copy(
            wall_mine, wall_all.at[index], wall_send.at[step - 1], wall_recv.at[index],
            device_id=device, device_id_type=MESH,
        )
        return send, receive

    for step in (1, 2, 3):
        wall_copy(step)[0].start()
    wall_all[me] = wall_mine[...]

    def ended(step, carry):
        for copy in halo_copies(step):
            copy.wait_send()
        for copy in mode_copies(step):
            copy.wait_send()
        return carry

    lax.fori_loop(0, STEPS, ended, 0)

    def ended_group(group, carry):
        for copy in coef_copies(group):
            copy.wait_send()
        return carry

    lax.fori_loop(0, GROUPS, ended_group, 0)
    for stage in range(3):
        for step in range(1, stage_size[stage]):
            sum_copies(stage, step)[0].wait_send()
    for step in (1, 2, 3):
        wall_copy(step)[0].wait_send()
        wall_copy(step)[1].wait_recv()
    wall_ref[...] = (wall_all[0] + wall_all[1]) + (wall_all[2] + wall_all[3])


def per_device(sizes, state, inverse):
    both, back = window_tables(PTS + 2 * HALO, HALO, PTS, MODES)
    project = jnp.asarray(np.concatenate(split_table(both), axis=0))
    high, low = split_table(back)
    back = jnp.asarray(np.concatenate([high, high, low], axis=0))
    exchange = (4, MEMBERS * BLOCK, PTS)
    rim = (MEMBERS, FIELDS, 32, PTS)
    vmem = pltpu.VMEM
    dma = pltpu.SemaphoreType.DMA
    updated, wall = pl.pallas_call(
        functools.partial(kernel, sizes),
        out_shape=(
            pltpu.VMEM(state.shape, F32),
            pltpu.VMEM((4 * MEMBERS, PTS), F32),
        ),
        in_specs=[pl.BlockSpec(memory_space=pl.ANY)] * 4,
        out_specs=(
            pl.BlockSpec(memory_space=pltpu.VMEM),
            pl.BlockSpec(memory_space=pltpu.VMEM),
        ),
        scratch_shapes=[
            vmem(state.shape, F32),
            vmem(inverse.shape, F32),
            vmem(inverse.shape, BF16),
            vmem(inverse.shape, BF16),
            vmem(project.shape, BF16),
            vmem(back.shape, BF16),
            *[vmem(rim, F32)] * 4,
            *[vmem(exchange, F32)] * 4,
            vmem((4, 1, PTS), F32),
            vmem((3, 8, 1, PTS), F32),
            vmem((4 * MEMBERS, PTS), F32),
            vmem((4, 4 * MEMBERS, PTS), F32),
            dma((7,)),
            dma((2, STEPS)),
            dma((2, STEPS)),
            dma((4, STEPS)),
            dma((4, STEPS)),
            dma((4, GROUPS)),
            dma((4, GROUPS)),
            dma((3, 7)),
            dma((3, 8)),
            dma((3,)),
            dma((4,)),
        ],
        compiler_params=pltpu.CompilerParams(
            collective_id=0, has_side_effects=True, vmem_limit_bytes=56 * 1024 * 1024
        ),
        name="step",
    )(state, inverse, project, back)
    return updated, wall.reshape(MEMBERS, 2, 2, PTS)


def solution(mesh):
    torus = Mesh(mesh.devices.reshape(4, 2, 8, 2, 2), AXES)
    return jax.shard_map(
        functools.partial(per_device, (4, 2, 8)),
        mesh=torus,
        in_specs=(P(None, None, GY, GX), P(GY, None, None)),
        out_specs=(P(None, None, GY, GX), P(None, None, None, GX)),
        check_vma=False,
    )
```

```python
import functools

import jax
import jax.numpy as jnp
import numpy as np
from jax import lax
from jax.experimental import pallas as pl
from jax.experimental.pallas import tpu as pltpu
from jax.sharding import Mesh
from jax.sharding import PartitionSpec as P

MODES = 128
HALO = 64
AXES = ("gx_0", "gx_1", "gx_2", "gy_0", "gy_1")
GX = ("gx_0", "gx_1", "gx_2")
GY = ("gy_0", "gy_1")
EPSILON = 1e-06
TIME_STEP = 0.5
MEAN_FLOW = 0.8
CORIOLIS = 0.6
STRATIFICATION = 0.9
F32 = jnp.float32
BF16 = jnp.bfloat16
MESH = pl.DeviceIdType.MESH

MEMBERS = 12
FIELDS = 4
LOCAL = 64
PTS = 128
QUARTER = 32
BLOCK = 2 * QUARTER
STEP = 2
STEPS = MEMBERS // STEP
GROUP = 4
GROUPS = MEMBERS // GROUP
UNROLL = 8


def window_tables(window, rim, points, modes):
    pos = np.arange(window)
    mode = np.arange(modes)
    half = modes // 2
    cosine = mode <= half
    wave = np.where(cosine, mode, mode - half)
    phase = 2.0 * np.pi * (pos[:, None] * wave[None, :] % window) / window
    norm = np.where(wave == 0, np.sqrt(1.0 / window), np.sqrt(2.0 / window))
    basis = np.where(cosine[None, :], np.cos(phase), np.sin(phase)) * norm[None, :]
    kappa = 2.0 * np.pi * wave / window
    paired = wave[:, None] == wave[None, :]
    to_sine = cosine[:, None] & ~cosine[None, :] & paired
    to_cosine = ~cosine[:, None] & cosine[None, :] & paired
    derivative = np.where(to_sine, -kappa[:, None], 0.0) + np.where(to_cosine, kappa[:, None], 0.0)
    taper = 0.25 + 0.75 * np.sin(np.pi * (pos + 0.5) / window) ** 2
    plain = basis * taper[:, None]
    slope = (basis @ derivative) * taper[:, None]
    both = np.concatenate([plain - TIME_STEP * MEAN_FLOW * slope, plain], axis=1).T
    order = np.concatenate([np.arange(rim, window), np.arange(rim)])
    back = (basis[rim : rim + points] / taper[rim : rim + points, None]).T
    return both[:, order], back


def split_table(table):
    high = table.astype(BF16)
    low = (table - high.astype(np.float64)).astype(BF16)
    return high, low


def split(a):
    high = a.astype(BF16)
    low = (a - high.astype(F32)).astype(BF16)
    return high, low


def dot_t(a, b):
    return lax.dot_general(a, b, (((1,), (1,)), ((), ())), preferred_element_type=F32)


def dot(a, b):
    return lax.dot_general(a, b, (((1,), (0,)), ((), ())), preferred_element_type=F32)


def kernel(
    sizes,
    state_hbm, inverse_hbm, project_hbm, back_hbm, out_ref, wall_ref,
    state, inverse, inv_high, inv_low, project, back,
    to_right, to_left, from_left, from_right,
    out_modes, in_modes, out_coefs, in_coefs,
    sum_mine, sum_all, wall_mine, wall_all,
    local_sem, halo_send, halo_recv, mode_send, mode_recv, coef_send, coef_recv,
    sum_send, sum_recv, wall_send, wall_recv,
):
    nx, ny, nz = sizes
    x, y, z = (lax.axis_index(a) for a in GX)
    hi, core = (lax.axis_index(a) for a in GY)
    me = hi * 2 + core
    count = nx * ny * nz
    here = (x * ny + y) * nz + z

    def place(index):
        return {
            "gx_0": lax.div(index, ny * nz),
            "gx_1": lax.rem(lax.div(index, nz), ny),
            "gx_2": lax.rem(index, nz),
        }

    right = place(lax.rem(here + 1, count))
    left = place(lax.rem(here + count - 1, count))
    solvers = [{"gx_1": 1 - y, "gy_0": q // 2, "gy_1": q % 2} for q in range(4)]

    def other(step):
        index = lax.rem(me + step, 4)
        return index, {"gy_0": lax.div(index, 2), "gy_1": lax.rem(index, 2)}

    def stage_peer(stage, step):
        if stage == 0:
            index = lax.rem(z + step, nz)
            return index, {"gx_2": index}
        if stage == 1:
            index = lax.rem(x + step, nx)
            return index, {"gx_0": index}
        index = lax.rem(y * 4 + me + step, 4 * ny)
        return index, {
            "gx_1": lax.div(index, 4),
            "gy_0": lax.rem(lax.div(index, 2), 2),
            "gy_1": lax.rem(index, 2),
        }

    stage_me = (z, x, y * 4 + me)
    stage_size = (nz, nx, 4 * ny)
    peers = [stage_peer(k, n)[1] for k in range(3) for n in range(1, stage_size[k])]

    upper = lax.div(z, nz // 2)
    depth = upper * (nz - 1 - z) + (1 - upper) * z
    inner = z + 1 - 2 * upper
    outer = z - 1 + 2 * upper

    def at_plane(device, plane):
        return {**device, "gx_2": plane}

    barrier = pltpu.get_barrier_semaphore()
    met = [right, left, *peers]
    for device in met:
        pl.semaphore_signal(barrier, inc=1, device_id=device, device_id_type=MESH)
    for level, plane in ((0, inner), (1, outer)):
        @pl.when(depth == level)
        def _():
            for device in solvers:
                pl.semaphore_signal(
                    barrier, inc=1, device_id=at_plane(device, plane), device_id_type=MESH
                )

    state_load = pltpu.make_async_copy(state_hbm, state, local_sem.at[0])
    state_load.start()
    loads = [
        pltpu.make_async_copy(project_hbm, project, local_sem.at[1]),
        pltpu.make_async_copy(back_hbm, back, local_sem.at[2]),
    ]
    for k in range(4):
        part = pl.ds(k * 8, 8)
        loads.append(
            pltpu.make_async_copy(inverse_hbm.at[part], inverse.at[part], local_sem.at[3 + k])
        )

    lane = lax.broadcasted_iota(jnp.int32, (1, PTS), 1)
    low_half = lane < LOCAL

    def halo_copies(step):
        rows = pl.ds(step * STEP, STEP)
        return (
            pltpu.make_async_remote_copy(
                to_right.at[rows], from_left.at[rows], halo_send.at[0, step], halo_recv.at[0, step],
                device_id=right, device_id_type=MESH,
            ),
            pltpu.make_async_remote_copy(
                to_left.at[rows], from_right.at[rows], halo_send.at[1, step], halo_recv.at[1, step],
                device_id=left, device_id_type=MESH,
            ),
        )

    state_load.wait()
    for load in loads:
        load.start()

    def pack(e):
        centre = state[e]
        top, low = centre[:, :32], centre[:, 32:]
        turned = pltpu.roll(low, LOCAL, 2)
        to_right[e] = jnp.where(low_half, turned, top)
        to_left[e] = jnp.where(low_half, top, turned)

    for k in range(STEP):
        pack(k)

    def squares(e, carry):
        values = state[e].reshape(FIELDS * LOCAL, PTS)
        total = jnp.sum(values * values, axis=0, keepdims=True)
        return jnp.where(lane == e, jnp.sum(total, axis=1, keepdims=True), carry)

    def sum_copies(stage, step):
        index, device = stage_peer(stage, step)

        def copy(slot):
            return pltpu.make_async_remote_copy(
                sum_mine.at[stage], sum_all.at[stage, slot],
                sum_send.at[stage, step - 1], sum_recv.at[stage, slot],
                device_id=device, device_id_type=MESH,
            )

        return copy(stage_me[stage]), copy(index)

    def sum_start(stage):
        for step in range(1, stage_size[stage]):
            sum_copies(stage, step)[0].start()
        sum_all[stage, stage_me[stage]] = sum_mine[stage]

    def sum_end(stage):
        for step in range(1, stage_size[stage]):
            sum_copies(stage, step)[1].wait_recv()
        total = sum_all[stage, 0]
        for k in range(1, stage_size[stage]):
            total = total + sum_all[stage, k]
        sum_mine[stage + 1] = total

    pl.semaphore_wait(barrier, len(met) + len(solvers) * (1 - lax.div(depth + 2, 4)))
    for copy in halo_copies(0):
        copy.start()
    sum_mine[0] = lax.fori_loop(0, MEMBERS, squares, jnp.zeros((1, PTS), F32))
    sum_start(0)

    def pack_and_send(step, carry):
        for k in range(STEP):
            pack(step * STEP + k)
        for copy in halo_copies(step):
            copy.start()
        return carry

    lax.fori_loop(1, STEPS, pack_and_send, 0)

    for load in loads:
        load.wait()

    def split_inverse(m, carry):
        high, low = split(inverse[m])
        inv_high[m] = high
        inv_low[m] = low
        return carry

    lax.fori_loop(0, QUARTER, split_inverse, 0)

    coupling_0 = jnp.where(low_half, TIME_STEP * CORIOLIS, TIME_STEP)
    coupling_1 = jnp.where(low_half, -TIME_STEP * CORIOLIS, -TIME_STEP * STRATIFICATION)
    coefficient = me * LOCAL + lax.rem(lane, LOCAL)
    interior = coefficient < 4 * LOCAL - 2

    def mode_copies(step):
        moved = lax.div(step, STEPS - STEP) * (1 - lax.div(depth + nz - 1, nz))
        target = step + moved * STEP
        rows = pl.ds(step * (STEP * BLOCK), STEP * BLOCK)
        target_rows = pl.ds(target * (STEP * BLOCK), STEP * BLOCK)
        return [
            pltpu.make_async_remote_copy(
                out_modes.at[q, rows], in_modes.at[me, target_rows],
                mode_send.at[q, step], mode_recv.at[me, target],
                device_id=at_plane(solvers[q], z + moved * (1 - 2 * upper)), device_id_type=MESH,
            )
            for q in range(4)
        ]

    def project_member(e):
        centre = state[e]
        rim_left, rim_right = from_left[e], from_right[e]
        top = jnp.where(low_half, rim_right, rim_left)
        low = pltpu.roll(jnp.where(low_half, rim_left, rim_right), LOCAL, 2)
        rim = jnp.concatenate([top, low], axis=1)
        segment = jnp.concatenate(
            [centre.reshape(FIELDS * LOCAL, PTS), rim.reshape(FIELDS * LOCAL, PTS)], axis=1
        )
        high, low = split(segment)
        first = dot_t(project[...], high)
        second = dot_t(project[: 2 * MODES], low)
        both = first[: 2 * MODES] + (first[2 * MODES :] + second)
        a_0, a_1 = both[:MODES, :PTS], both[:MODES, PTS:]
        b_0, b_1 = both[MODES:, :PTS], both[MODES:, PTS:]
        rhs_0 = jnp.where(interior, a_0 + coupling_0 * b_1, 0.0)
        rhs_1 = jnp.where(interior, a_1 + coupling_1 * b_0, 0.0)
        for q in range(4):
            modes = slice(q * QUARTER, (q + 1) * QUARTER)
            base = pl.multiple_of(e * BLOCK, BLOCK)
            out_modes[q, pl.ds(base, QUARTER), :] = rhs_0[modes]
            out_modes[q, pl.ds(base + QUARTER, QUARTER), :] = rhs_1[modes]

    def project_step(step, carry):
        for copy in halo_copies(step):
            copy.wait_recv()
        for k in range(STEP):
            project_member(step * STEP + k)
        for copy in mode_copies(step):
            copy.start()

        @pl.when(step == 2)
        def _():
            sum_end(0)
            sum_start(1)

        @pl.when(step == 4)
        def _():
            sum_end(1)
            sum_start(2)

        return carry

    lax.fori_loop(0, STEPS, project_step, 0)

    def coef_copies(slot):
        moved = lax.div(slot, GROUPS)
        group = slot - moved
        rows = pl.ds(slot * (GROUP * BLOCK), GROUP * BLOCK)
        target_rows = pl.ds(group * (GROUP * BLOCK), GROUP * BLOCK)
        return [
            pltpu.make_async_remote_copy(
                out_coefs.at[t, rows], in_coefs.at[me, target_rows],
                coef_send.at[t, slot], coef_recv.at[me, group],
                device_id=at_plane(solvers[t], z + moved * (2 * upper - 1)), device_id_type=MESH,
            )
            for t in range(4)
        ]

    def solved_here(slot):
        return (slot < GROUPS - 1) | ((slot == GROUPS - 1) & (depth > 0)) | ((slot == GROUPS) & (depth == 1))

    def arrived(buffer, sem, rows, s, k):
        return pltpu.make_async_remote_copy(
            buffer.at[s, rows], buffer.at[s, rows], sem.at[s, k], sem.at[s, k],
            device_id=solvers[s], device_id_type=MESH,
        )

    def turn(a):
        return pltpu.roll(a, LOCAL, 1)

    def solve_mode(base, m):
        rows = pl.ds(base + m, 2 * GROUP, stride=QUARTER)
        parts = [in_modes[s, rows, :] for s in range(4)]
        even, odd = [], []
        for s in (0, 2):
            first, second = parts[s], parts[s + 1]
            even.append(jnp.where(low_half, first, turn(second)))
            odd.append(jnp.where(low_half, turn(first), second))
        values = jnp.concatenate(
            [jnp.concatenate(even, axis=1), jnp.concatenate(odd, axis=1)], axis=0
        )
        high, low = split(values)
        count = 4 * GROUP
        first = dot_t(jnp.concatenate([high, low], axis=0), inv_high[m])
        second = dot_t(high, inv_low[m])
        solved = first[:count] + (first[count:] + second)
        even, odd = solved[: 2 * GROUP], solved[2 * GROUP :]
        for k in range(2):
            lanes = slice(k * PTS, (k + 1) * PTS)
            out_coefs[2 * k, rows, :] = jnp.where(low_half, even[:, lanes], turn(odd[:, lanes]))
            out_coefs[2 * k + 1, rows, :] = jnp.where(low_half, turn(even[:, lanes]), odd[:, lanes])

    def solve_group(group):
        for s in range(4):
            for k in range(GROUP // STEP):
                step = group * (GROUP // STEP) + k
                rows = pl.ds(step * (STEP * BLOCK), STEP * BLOCK)
                arrived(in_modes, mode_recv, rows, s, step).wait_recv()
        base = group * (GROUP * BLOCK)

        def some_modes(k, carry):
            for u in range(UNROLL):
                solve_mode(base, k * UNROLL + u)
            return carry

        lax.fori_loop(0, QUARTER // UNROLL, some_modes, 0)
        for copy in coef_copies(group):
            copy.start()

    def solve_slot(slot, carry):
        @pl.when(solved_here(slot))
        def _():
            solve_group(slot)

        return carry

    lax.fori_loop(0, GROUPS + 1, solve_slot, 0)

    row = lax.broadcasted_iota(jnp.int32, (LOCAL, PTS), 0)
    k_float = (me * LOCAL + row).astype(F32)
    curvature = k_float * k_float / float((4 * LOCAL) ** 2)
    parity = jnp.where(lax.rem(row[:8], 2) == 0, -1.0, 1.0)
    grid = float(FIELDS * 4 * LOCAL * PTS * count)

    sum_end(2)

    def back_member(e):
        base = pl.multiple_of(e * BLOCK, BLOCK)
        turned = []
        for col in range(2):
            block = jnp.concatenate(
                [in_coefs[q, pl.ds(base + col * QUARTER, QUARTER), :] for q in range(4)], axis=0
            )
            turned.append(block.T)
        high, low = split(jnp.concatenate(turned, axis=0))
        values = dot(jnp.concatenate([high, low], axis=1), back[: 2 * MODES])
        values = values + dot(high, back[2 * MODES :])
        total = jnp.sum(jnp.where(lane == e, sum_mine[3], 0.0), axis=1, keepdims=True)
        values = values * lax.rsqrt(total / grid + EPSILON)
        out_ref[e] = values.reshape(FIELDS, LOCAL, PTS)
        for c in range(2):
            weighted = values[c * PTS : c * PTS + LOCAL] * curvature
            rows = jnp.sum(weighted.reshape(LOCAL // 8, 8, PTS), axis=0)
            wall_mine[pl.ds(e * 4 + c, 1), :] = jnp.sum(rows, axis=0, keepdims=True)
            wall_mine[pl.ds(e * 4 + 2 + c, 1), :] = jnp.sum(rows * parity, axis=0, keepdims=True)

    def back_group(group, carry):
        rows = pl.ds(group * (GROUP * BLOCK), GROUP * BLOCK)
        for s in range(4):
            arrived(in_coefs, coef_recv, rows, s, group).wait_recv()

        def one(k, carry):
            back_member(group * GROUP + k)
            return carry

        lax.fori_loop(0, GROUP, one, 0)
        return carry

    lax.fori_loop(0, GROUPS, back_group, 0)

    def wall_copy(step):
        index, device = other(step)
        send = pltpu.make_async_remote_copy(
            wall_mine, wall_all.at[me], wall_send.at[step - 1], wall_recv.at[me],
            device_id=device, device_id_type=MESH,
        )
        receive = pltpu.make_async_remote_copy(
            wall_mine, wall_all.at[index], wall_send.at[step - 1], wall_recv.at[index],
            device_id=device, device_id_type=MESH,
        )
        return send, receive

    for step in (1, 2, 3):
        wall_copy(step)[0].start()
    wall_all[me] = wall_mine[...]

    def ended(step, carry):
        for copy in halo_copies(step):
            copy.wait_send()
        for copy in mode_copies(step):
            copy.wait_send()
        return carry

    lax.fori_loop(0, STEPS, ended, 0)

    def ended_group(group, carry):
        @pl.when(solved_here(group))
        def _():
            for copy in coef_copies(group):
                copy.wait_send()

        return carry

    lax.fori_loop(0, GROUPS + 1, ended_group, 0)
    for stage in range(3):
        for step in range(1, stage_size[stage]):
            sum_copies(stage, step)[0].wait_send()
    for step in (1, 2, 3):
        wall_copy(step)[0].wait_send()
        wall_copy(step)[1].wait_recv()
    wall_ref[...] = (wall_all[0] + wall_all[1]) + (wall_all[2] + wall_all[3])


def per_device(sizes, state, inverse):
    both, back = window_tables(PTS + 2 * HALO, HALO, PTS, MODES)
    project = jnp.asarray(np.concatenate(split_table(both), axis=0))
    high, low = split_table(back)
    back = jnp.asarray(np.concatenate([high, high, low], axis=0))
    exchange = (4, MEMBERS * BLOCK, PTS)
    larger = (4, (MEMBERS + GROUP) * BLOCK, PTS)
    rim = (MEMBERS, FIELDS, 32, PTS)
    vmem = pltpu.VMEM
    dma = pltpu.SemaphoreType.DMA
    updated, wall = pl.pallas_call(
        functools.partial(kernel, sizes),
        out_shape=(
            pltpu.VMEM(state.shape, F32),
            pltpu.VMEM((4 * MEMBERS, PTS), F32),
        ),
        in_specs=[pl.BlockSpec(memory_space=pl.ANY)] * 4,
        out_specs=(
            pl.BlockSpec(memory_space=pltpu.VMEM),
            pl.BlockSpec(memory_space=pltpu.VMEM),
        ),
        scratch_shapes=[
            vmem(state.shape, F32),
            vmem(inverse.shape, F32),
            vmem(inverse.shape, BF16),
            vmem(inverse.shape, BF16),
            vmem(project.shape, BF16),
            vmem(back.shape, BF16),
            *[vmem(rim, F32)] * 4,
            vmem(exchange, F32),
            vmem(larger, F32),
            vmem(larger, F32),
            vmem(exchange, F32),
            vmem((4, 1, PTS), F32),
            vmem((3, 8, 1, PTS), F32),
            vmem((4 * MEMBERS, PTS), F32),
            vmem((4, 4 * MEMBERS, PTS), F32),
            dma((7,)),
            dma((2, STEPS)),
            dma((2, STEPS)),
            dma((4, STEPS)),
            dma((4, STEPS + GROUP // STEP)),
            dma((4, GROUPS + 1)),
            dma((4, GROUPS)),
            dma((3, 7)),
            dma((3, 8)),
            dma((3,)),
            dma((4,)),
        ],
        compiler_params=pltpu.CompilerParams(
            collective_id=0, has_side_effects=True, vmem_limit_bytes=56 * 1024 * 1024
        ),
        name="step",
    )(state, inverse, project, back)
    return updated, wall.reshape(MEMBERS, 2, 2, PTS)


def solution(mesh):
    torus = Mesh(mesh.devices.reshape(4, 2, 8, 2, 2), AXES)
    return jax.shard_map(
        functools.partial(per_device, (4, 2, 8)),
        mesh=torus,
        in_specs=(P(None, None, GY, GX), P(GY, None, None)),
        out_specs=(P(None, None, GY, GX), P(None, None, None, GX)),
        check_vma=False,
    )
```

```python
import functools

import jax
import jax.numpy as jnp
import numpy as np
from jax import lax
from jax.experimental import pallas as pl
from jax.experimental.pallas import tpu as pltpu
from jax.sharding import Mesh
from jax.sharding import PartitionSpec as P

MODES = 128
HALO = 64
AXES = ("gx_0", "gx_1", "gx_2", "gy_0", "gy_1")
GX = ("gx_0", "gx_1", "gx_2")
GY = ("gy_0", "gy_1")
EPSILON = 1e-06
TIME_STEP = 0.5
MEAN_FLOW = 0.8
CORIOLIS = 0.6
STRATIFICATION = 0.9
F32 = jnp.float32
BF16 = jnp.bfloat16
MESH = pl.DeviceIdType.MESH

MEMBERS = 12
FIELDS = 4
LOCAL = 64
PTS = 128
QUARTER = 32
BLOCK = 2 * QUARTER
STEP = 2
STEPS = MEMBERS // STEP
GROUP = 4
GROUPS = MEMBERS // GROUP
UNROLL = 8


def window_tables(window, rim, points, modes):
    pos = np.arange(window)
    mode = np.arange(modes)
    half = modes // 2
    cosine = mode <= half
    wave = np.where(cosine, mode, mode - half)
    phase = 2.0 * np.pi * (pos[:, None] * wave[None, :] % window) / window
    norm = np.where(wave == 0, np.sqrt(1.0 / window), np.sqrt(2.0 / window))
    basis = np.where(cosine[None, :], np.cos(phase), np.sin(phase)) * norm[None, :]
    kappa = 2.0 * np.pi * wave / window
    paired = wave[:, None] == wave[None, :]
    to_sine = cosine[:, None] & ~cosine[None, :] & paired
    to_cosine = ~cosine[:, None] & cosine[None, :] & paired
    derivative = np.where(to_sine, -kappa[:, None], 0.0) + np.where(to_cosine, kappa[:, None], 0.0)
    taper = 0.25 + 0.75 * np.sin(np.pi * (pos + 0.5) / window) ** 2
    plain = basis * taper[:, None]
    slope = (basis @ derivative) * taper[:, None]
    both = np.concatenate([plain - TIME_STEP * MEAN_FLOW * slope, plain], axis=1).T
    order = np.concatenate([np.arange(rim, window), np.arange(rim)])
    back = (basis[rim : rim + points] / taper[rim : rim + points, None]).T
    return both[:, order], back


def split_table(table):
    high = table.astype(BF16)
    low = (table - high.astype(np.float64)).astype(BF16)
    return high, low


def split(a):
    high = a.astype(BF16)
    low = (a - high.astype(F32)).astype(BF16)
    return high, low


def dot_t(a, b):
    return lax.dot_general(a, b, (((1,), (1,)), ((), ())), preferred_element_type=F32)


def dot(a, b):
    return lax.dot_general(a, b, (((1,), (0,)), ((), ())), preferred_element_type=F32)


def kernel(
    sizes,
    state_hbm, inverse_hbm, project_hbm, back_hbm, weights_hbm, out_ref, wall_ref,
    state, inverse, inv_high, inv_low, project, back, weights,
    to_right, to_left, from_left, from_right,
    out_modes, in_modes, out_coefs, in_coefs,
    sum_mine, sum_all, wall_out, wall_in,
    local_sem, halo_send, halo_recv, mode_send, mode_recv, coef_send, coef_recv,
    sum_send, sum_recv, wall_send, wall_recv,
):
    nx, ny, nz = sizes
    x, y, z = (lax.axis_index(a) for a in GX)
    hi, core = (lax.axis_index(a) for a in GY)
    me = hi * 2 + core
    count = nx * ny * nz
    here = (x * ny + y) * nz + z

    def place(index):
        return {
            "gx_0": lax.div(index, ny * nz),
            "gx_1": lax.rem(lax.div(index, nz), ny),
            "gx_2": lax.rem(index, nz),
        }

    right = place(lax.rem(here + 1, count))
    left = place(lax.rem(here + count - 1, count))
    solvers = [{"gx_1": 1 - y, "gy_0": q // 2, "gy_1": q % 2} for q in range(4)]

    def stage_peer(stage, step):
        if stage == 0:
            index = lax.rem(z + step, nz)
            return index, {"gx_2": index}
        if stage == 1:
            index = lax.rem(x + step, nx)
            return index, {"gx_0": index}
        index = lax.rem(y * 4 + me + step, 4 * ny)
        return index, {
            "gx_1": lax.div(index, 4),
            "gy_0": lax.rem(lax.div(index, 2), 2),
            "gy_1": lax.rem(index, 2),
        }

    stage_me = (z, x, y * 4 + me)
    stage_size = (nz, nx, 4 * ny)
    peers = [stage_peer(k, n)[1] for k in range(3) for n in range(1, stage_size[k])]

    upper = lax.div(z, nz // 2)
    depth = upper * (nz - 1 - z) + (1 - upper) * z
    inner = z + 1 - 2 * upper
    outer = z - 1 + 2 * upper

    def at_plane(device, plane):
        return {**device, "gx_2": plane}

    barrier = pltpu.get_barrier_semaphore()
    met = [right, left, *peers]
    for device in met:
        pl.semaphore_signal(barrier, inc=1, device_id=device, device_id_type=MESH)
    for level, plane in ((0, inner), (1, outer)):
        @pl.when(depth == level)
        def _():
            for device in solvers:
                pl.semaphore_signal(
                    barrier, inc=1, device_id=at_plane(device, plane), device_id_type=MESH
                )

    state_load = pltpu.make_async_copy(state_hbm, state, local_sem.at[0])
    state_load.start()
    loads = [
        pltpu.make_async_copy(project_hbm, project, local_sem.at[1]),
        pltpu.make_async_copy(back_hbm, back, local_sem.at[2]),
        pltpu.make_async_copy(weights_hbm, weights, local_sem.at[7]),
    ]
    for k in range(4):
        part = pl.ds(k * 8, 8)
        loads.append(
            pltpu.make_async_copy(inverse_hbm.at[part], inverse.at[part], local_sem.at[3 + k])
        )

    lane = lax.broadcasted_iota(jnp.int32, (1, PTS), 1)
    low_half = lane < LOCAL

    def halo_copies(step):
        rows = pl.ds(step * STEP, STEP)
        return (
            pltpu.make_async_remote_copy(
                to_right.at[rows], from_left.at[rows], halo_send.at[0, step], halo_recv.at[0, step],
                device_id=right, device_id_type=MESH,
            ),
            pltpu.make_async_remote_copy(
                to_left.at[rows], from_right.at[rows], halo_send.at[1, step], halo_recv.at[1, step],
                device_id=left, device_id_type=MESH,
            ),
        )

    state_load.wait()
    for load in loads:
        load.start()

    def pack(e):
        centre = state[e]
        top, low = centre[:, :32], centre[:, 32:]
        turned = pltpu.roll(low, LOCAL, 2)
        to_right[e] = jnp.where(low_half, turned, top)
        to_left[e] = jnp.where(low_half, top, turned)

    for k in range(STEP):
        pack(k)

    def squares(e, carry):
        values = state[e].reshape(FIELDS * LOCAL, PTS)
        total = jnp.sum(values * values, axis=0, keepdims=True)
        return jnp.where(lane == e, jnp.sum(total, axis=1, keepdims=True), carry)

    def sum_copies(stage, step):
        index, device = stage_peer(stage, step)

        def copy(slot):
            return pltpu.make_async_remote_copy(
                sum_mine.at[stage], sum_all.at[stage, slot],
                sum_send.at[stage, step - 1], sum_recv.at[stage, slot],
                device_id=device, device_id_type=MESH,
            )

        return copy(stage_me[stage]), copy(index)

    def sum_start(stage):
        for step in range(1, stage_size[stage]):
            sum_copies(stage, step)[0].start()
        sum_all[stage, stage_me[stage]] = sum_mine[stage]

    def sum_end(stage):
        for step in range(1, stage_size[stage]):
            sum_copies(stage, step)[1].wait_recv()
        total = sum_all[stage, 0]
        for k in range(1, stage_size[stage]):
            total = total + sum_all[stage, k]
        sum_mine[stage + 1] = total

    pl.semaphore_wait(barrier, len(met) + len(solvers) * (1 - lax.div(depth + 2, 4)))
    for copy in halo_copies(0):
        copy.start()
    sum_mine[0] = lax.fori_loop(0, MEMBERS, squares, jnp.zeros((1, PTS), F32))
    sum_start(0)

    def pack_and_send(step, carry):
        for k in range(STEP):
            pack(step * STEP + k)
        for copy in halo_copies(step):
            copy.start()
        return carry

    lax.fori_loop(1, STEPS, pack_and_send, 0)

    for load in loads:
        load.wait()

    def split_inverse(m, carry):
        high, low = split(inverse[m])
        inv_high[m] = high
        inv_low[m] = low
        return carry

    lax.fori_loop(0, QUARTER, split_inverse, 0)

    coupling_0 = jnp.where(low_half, TIME_STEP * CORIOLIS, TIME_STEP)
    coupling_1 = jnp.where(low_half, -TIME_STEP * CORIOLIS, -TIME_STEP * STRATIFICATION)
    coefficient = me * LOCAL + lax.rem(lane, LOCAL)
    interior = coefficient < 4 * LOCAL - 2

    def mode_copies(step):
        moved = lax.div(step, STEPS - STEP) * (1 - lax.div(depth + nz - 1, nz))
        target = step + moved * STEP
        rows = pl.ds(step * (STEP * BLOCK), STEP * BLOCK)
        target_rows = pl.ds(target * (STEP * BLOCK), STEP * BLOCK)
        return [
            pltpu.make_async_remote_copy(
                out_modes.at[q, rows], in_modes.at[me, target_rows],
                mode_send.at[q, step], mode_recv.at[me, target],
                device_id=at_plane(solvers[q], z + moved * (1 - 2 * upper)), device_id_type=MESH,
            )
            for q in range(4)
        ]

    def project_member(e):
        centre = state[e]
        rim_left, rim_right = from_left[e], from_right[e]
        top = jnp.where(low_half, rim_right, rim_left)
        low = pltpu.roll(jnp.where(low_half, rim_left, rim_right), LOCAL, 2)
        rim = jnp.concatenate([top, low], axis=1)
        segment = jnp.concatenate(
            [centre.reshape(FIELDS * LOCAL, PTS), rim.reshape(FIELDS * LOCAL, PTS)], axis=1
        )
        high, low = split(segment)
        first = dot_t(project[...], high)
        second = dot_t(project[: 2 * MODES], low)
        both = first[: 2 * MODES] + (first[2 * MODES :] + second)
        a_0, a_1 = both[:MODES, :PTS], both[:MODES, PTS:]
        b_0, b_1 = both[MODES:, :PTS], both[MODES:, PTS:]
        rhs_0 = jnp.where(interior, a_0 + coupling_0 * b_1, 0.0)
        rhs_1 = jnp.where(interior, a_1 + coupling_1 * b_0, 0.0)
        for q in range(4):
            modes = slice(q * QUARTER, (q + 1) * QUARTER)
            base = pl.multiple_of(e * BLOCK, BLOCK)
            out_modes[q, pl.ds(base, QUARTER), :] = rhs_0[modes]
            out_modes[q, pl.ds(base + QUARTER, QUARTER), :] = rhs_1[modes]

    def project_step(step, carry):
        for copy in halo_copies(step):
            copy.wait_recv()
        for k in range(STEP):
            project_member(step * STEP + k)
        for copy in mode_copies(step):
            copy.start()

        @pl.when(step == 2)
        def _():
            sum_end(0)
            sum_start(1)

        @pl.when(step == 4)
        def _():
            sum_end(1)
            sum_start(2)

        return carry

    lax.fori_loop(0, STEPS, project_step, 0)

    def back_to(slot, t):
        return at_plane(solvers[t], z + lax.div(slot, GROUPS) * (2 * upper - 1))

    def coef_copies(step):
        slot = lax.div(step, GROUP // STEP)
        moved = lax.div(slot, GROUPS)
        target = step - moved * (GROUP // STEP)
        rows = pl.ds(step * (STEP * BLOCK), STEP * BLOCK)
        target_rows = pl.ds(target * (STEP * BLOCK), STEP * BLOCK)
        return [
            pltpu.make_async_remote_copy(
                out_coefs.at[t, rows], in_coefs.at[me, target_rows],
                coef_send.at[t, step], coef_recv.at[me, target],
                device_id=back_to(slot, t), device_id_type=MESH,
            )
            for t in range(4)
        ]

    def wall_copies(slot):
        group = slot - lax.div(slot, GROUPS)
        return [
            pltpu.make_async_remote_copy(
                wall_out.at[slot], wall_in.at[me, group],
                wall_send.at[t, slot], wall_recv.at[me, group],
                device_id=back_to(slot, t), device_id_type=MESH,
            )
            for t in range(4)
        ]

    def wall_arrived(q, group):
        return pltpu.make_async_remote_copy(
            wall_in.at[q, group], wall_in.at[q, group],
            wall_recv.at[q, group], wall_recv.at[q, group],
            device_id=solvers[q], device_id_type=MESH,
        )

    def wall_sums(slot):
        rows = pl.ds(slot * (GROUP * BLOCK), GROUP * BLOCK)
        blocks = jnp.concatenate([out_coefs[t, rows, :] for t in range(4)], axis=1)
        high, low = split(blocks)
        first = dot_t(weights[...], high)
        second = dot_t(weights[:16], low)
        wall_out[slot] = (first[:16] + (first[16:] + second))[:2]

    def solved_here(slot):
        return (slot < GROUPS - 1) | ((slot == GROUPS - 1) & (depth > 0)) | ((slot == GROUPS) & (depth == 1))

    def arrived(buffer, sem, rows, s, k):
        return pltpu.make_async_remote_copy(
            buffer.at[s, rows], buffer.at[s, rows], sem.at[s, k], sem.at[s, k],
            device_id=solvers[s], device_id_type=MESH,
        )

    def turn(a):
        return pltpu.roll(a, LOCAL, 1)

    def solve_mode(base, m):
        rows = pl.ds(base + m, 2 * GROUP, stride=QUARTER)
        parts = [in_modes[s, rows, :] for s in range(4)]
        even, odd = [], []
        for s in (0, 2):
            first, second = parts[s], parts[s + 1]
            even.append(jnp.where(low_half, first, turn(second)))
            odd.append(jnp.where(low_half, turn(first), second))
        values = jnp.concatenate(
            [jnp.concatenate(even, axis=1), jnp.concatenate(odd, axis=1)], axis=0
        )
        high, low = split(values)
        count = 4 * GROUP
        first = dot_t(jnp.concatenate([high, low], axis=0), inv_high[m])
        second = dot_t(high, inv_low[m])
        solved = first[:count] + (first[count:] + second)
        even, odd = solved[: 2 * GROUP], solved[2 * GROUP :]
        for k in range(2):
            lanes = slice(k * PTS, (k + 1) * PTS)
            out_coefs[2 * k, rows, :] = jnp.where(low_half, even[:, lanes], turn(odd[:, lanes]))
            out_coefs[2 * k + 1, rows, :] = jnp.where(low_half, turn(even[:, lanes]), odd[:, lanes])

    def solve_group(group):
        for s in range(4):
            for k in range(GROUP // STEP):
                step = group * (GROUP // STEP) + k
                rows = pl.ds(step * (STEP * BLOCK), STEP * BLOCK)
                arrived(in_modes, mode_recv, rows, s, step).wait_recv()
        base = group * (GROUP * BLOCK)

        def some_modes(k, carry):
            for u in range(UNROLL):
                solve_mode(base, k * UNROLL + u)
            return carry

        lax.fori_loop(0, QUARTER // UNROLL, some_modes, 0)
        for k in range(GROUP // STEP):
            for copy in coef_copies(group * (GROUP // STEP) + k):
                copy.start()
        wall_sums(group)
        for copy in wall_copies(group):
            copy.start()

    def solve_slot(slot, carry):
        @pl.when(solved_here(slot))
        def _():
            solve_group(slot)

        return carry

    lax.fori_loop(0, GROUPS + 1, solve_slot, 0)

    grid = float(FIELDS * 4 * LOCAL * PTS * count)

    sum_end(2)

    def back_member(e):
        base = pl.multiple_of(e * BLOCK, BLOCK)
        turned = []
        for col in range(2):
            block = jnp.concatenate(
                [in_coefs[q, pl.ds(base + col * QUARTER, QUARTER), :] for q in range(4)], axis=0
            )
            turned.append(block.T)
        high, low = split(jnp.concatenate(turned, axis=0))
        values = dot(jnp.concatenate([high, low], axis=1), back[: 2 * MODES])
        values = values + dot(high, back[2 * MODES : 3 * MODES])
        total = jnp.sum(jnp.where(lane == e, sum_mine[3], 0.0), axis=1, keepdims=True)
        values = values * lax.rsqrt(total / grid + EPSILON)
        out_ref[e] = values.reshape(FIELDS, LOCAL, PTS)

    row = lax.broadcasted_iota(jnp.int32, (4 * GROUP, 2 * PTS), 0)
    lanes = lax.broadcasted_iota(jnp.int32, (4 * GROUP, 2 * PTS), 1)
    own = lax.div(lanes, QUARTER) == 2 * lax.div(row, 4) + lax.rem(row, 2)
    upper_wall = lax.rem(lax.div(row, 2), 2) == 0

    def wall_group(group):
        parts = []
        for q in range(4):
            wall_arrived(q, group).wait_recv()
            both = wall_in[q, group]
            parts.append(jnp.where(own, jnp.where(upper_wall, both[:1], both[1:]), 0.0))
        high, low = split(jnp.concatenate(parts, axis=1))
        table = back[3 * MODES : 11 * MODES]
        first = dot(jnp.concatenate([high, low], axis=0), table)
        count = 4 * GROUP
        values = first[:count] + (first[count:] + dot(high, back[11 * MODES :]))
        member = group * GROUP + lax.div(row[:, :PTS], 4)
        total = jnp.sum(jnp.where(lane == member, sum_mine[3], 0.0), axis=1, keepdims=True)
        values = values * lax.rsqrt(total / grid + EPSILON)
        wall_ref[pl.ds(pl.multiple_of(group * count, count), count), :] = values

    def back_step(step, carry):
        rows = pl.ds(step * (STEP * BLOCK), STEP * BLOCK)
        for s in range(4):
            arrived(in_coefs, coef_recv, rows, s, step).wait_recv()
        for k in range(STEP):
            back_member(step * STEP + k)

        @pl.when(lax.rem(step, 2) == 1)
        def _():
            wall_group(lax.div(step, 2))

        return carry

    lax.fori_loop(0, STEPS, back_step, 0)

    def ended(step, carry):
        for copy in halo_copies(step):
            copy.wait_send()
        for copy in mode_copies(step):
            copy.wait_send()
        return carry

    lax.fori_loop(0, STEPS, ended, 0)

    def ended_group(group, carry):
        @pl.when(solved_here(group))
        def _():
            for k in range(GROUP // STEP):
                for copy in coef_copies(group * (GROUP // STEP) + k):
                    copy.wait_send()
            for copy in wall_copies(group):
                copy.wait_send()

        return carry

    lax.fori_loop(0, GROUPS + 1, ended_group, 0)
    for stage in range(3):
        for step in range(1, stage_size[stage]):
            sum_copies(stage, step)[0].wait_send()


def per_device(sizes, state, inverse):
    both, back = window_tables(PTS + 2 * HALO, HALO, PTS, MODES)
    project = jnp.asarray(np.concatenate(split_table(both), axis=0))
    high, low = split_table(back)

    def tiled(table):
        quarters = table.reshape(4, QUARTER, PTS)
        return np.concatenate([q for part in quarters for q in [part] * (2 * GROUP)], axis=0)

    back = jnp.asarray(np.concatenate([high, high, low, tiled(high), tiled(low)], axis=0))
    k = np.arange(4 * LOCAL, dtype=np.float64)
    curvature = k * k / (4 * LOCAL) ** 2
    walls = np.zeros((16, 4, 2, LOCAL))
    walls[0, :, 0] = curvature.reshape(4, LOCAL)
    walls[1, :, 0] = np.where(k % 2 == 0, -curvature, curvature).reshape(4, LOCAL)
    weights = jnp.asarray(np.concatenate(split_table(walls.reshape(16, 8 * LOCAL)), axis=0))
    exchange = (4, MEMBERS * BLOCK, PTS)
    larger = (4, (MEMBERS + GROUP) * BLOCK, PTS)
    rim = (MEMBERS, FIELDS, 32, PTS)
    vmem = pltpu.VMEM
    dma = pltpu.SemaphoreType.DMA
    updated, wall = pl.pallas_call(
        functools.partial(kernel, sizes),
        out_shape=(
            pltpu.VMEM(state.shape, F32),
            pltpu.VMEM((4 * MEMBERS, PTS), F32),
        ),
        in_specs=[pl.BlockSpec(memory_space=pl.ANY)] * 5,
        out_specs=(
            pl.BlockSpec(memory_space=pltpu.VMEM),
            pl.BlockSpec(memory_space=pltpu.VMEM),
        ),
        scratch_shapes=[
            vmem(state.shape, F32),
            vmem(inverse.shape, F32),
            vmem(inverse.shape, BF16),
            vmem(inverse.shape, BF16),
            vmem(project.shape, BF16),
            vmem(back.shape, BF16),
            vmem(weights.shape, BF16),
            *[vmem(rim, F32)] * 4,
            vmem(exchange, F32),
            vmem(larger, F32),
            vmem(larger, F32),
            vmem(exchange, F32),
            vmem((4, 1, PTS), F32),
            vmem((3, 8, 1, PTS), F32),
            vmem((GROUPS + 1, 2, 2 * PTS), F32),
            vmem((4, GROUPS, 2, 2 * PTS), F32),
            dma((8,)),
            dma((2, STEPS)),
            dma((2, STEPS)),
            dma((4, STEPS)),
            dma((4, STEPS + GROUP // STEP)),
            dma((4, STEPS + GROUP // STEP)),
            dma((4, STEPS)),
            dma((3, 7)),
            dma((3, 8)),
            dma((4, GROUPS + 1)),
            dma((4, GROUPS)),
        ],
        compiler_params=pltpu.CompilerParams(
            collective_id=0, has_side_effects=True, vmem_limit_bytes=56 * 1024 * 1024
        ),
        name="step",
    )(state, inverse, project, back, weights)
    return updated, wall.reshape(MEMBERS, 2, 2, PTS)


def solution(mesh):
    torus = Mesh(mesh.devices.reshape(4, 2, 8, 2, 2), AXES)
    return jax.shard_map(
        functools.partial(per_device, (4, 2, 8)),
        mesh=torus,
        in_specs=(P(None, None, GY, GX), P(GY, None, None)),
        out_specs=(P(None, None, GY, GX), P(None, None, None, GX)),
        check_vma=False,
    )
```

```python
import functools

import jax
import jax.numpy as jnp
import numpy as np
from jax import lax
from jax.experimental import pallas as pl
from jax.experimental.pallas import tpu as pltpu
from jax.sharding import Mesh
from jax.sharding import PartitionSpec as P

MODES = 128
HALO = 64
AXES = ("gx_0", "gx_1", "gx_2", "gy_0", "gy_1")
GX = ("gx_0", "gx_1", "gx_2")
GY = ("gy_0", "gy_1")
EPSILON = 1e-06
TIME_STEP = 0.5
MEAN_FLOW = 0.8
CORIOLIS = 0.6
STRATIFICATION = 0.9
F32 = jnp.float32
BF16 = jnp.bfloat16
MESH = pl.DeviceIdType.MESH

MEMBERS = 12
FIELDS = 4
LOCAL = 64
PTS = 128
QUARTER = 32
BLOCK = 2 * QUARTER
STEP = 2
STEPS = MEMBERS // STEP
GROUP = 4
GROUPS = MEMBERS // GROUP
UNROLL = 8
PIECES = QUARTER // UNROLL


def window_tables(window, rim, points, modes):
    pos = np.arange(window)
    mode = np.arange(modes)
    half = modes // 2
    cosine = mode <= half
    wave = np.where(cosine, mode, mode - half)
    phase = 2.0 * np.pi * (pos[:, None] * wave[None, :] % window) / window
    norm = np.where(wave == 0, np.sqrt(1.0 / window), np.sqrt(2.0 / window))
    basis = np.where(cosine[None, :], np.cos(phase), np.sin(phase)) * norm[None, :]
    kappa = 2.0 * np.pi * wave / window
    paired = wave[:, None] == wave[None, :]
    to_sine = cosine[:, None] & ~cosine[None, :] & paired
    to_cosine = ~cosine[:, None] & cosine[None, :] & paired
    derivative = np.where(to_sine, -kappa[:, None], 0.0) + np.where(to_cosine, kappa[:, None], 0.0)
    taper = 0.25 + 0.75 * np.sin(np.pi * (pos + 0.5) / window) ** 2
    plain = basis * taper[:, None]
    slope = (basis @ derivative) * taper[:, None]
    both = np.concatenate([plain - TIME_STEP * MEAN_FLOW * slope, plain], axis=1).T
    order = np.concatenate([np.arange(rim, window), np.arange(rim)])
    back = (basis[rim : rim + points] / taper[rim : rim + points, None]).T
    return both[:, order], back


def split_table(table):
    high = table.astype(BF16)
    low = (table - high.astype(np.float64)).astype(BF16)
    return high, low


def split(a):
    high = a.astype(BF16)
    low = (a - high.astype(F32)).astype(BF16)
    return high, low


def dot_t(a, b):
    return lax.dot_general(a, b, (((1,), (1,)), ((), ())), preferred_element_type=F32)


def dot(a, b):
    return lax.dot_general(a, b, (((1,), (0,)), ((), ())), preferred_element_type=F32)


def kernel(
    sizes,
    state_hbm, inverse_hbm, project_hbm, back_hbm, weights_hbm, out_ref, wall_ref,
    state, inverse, inv_high, inv_low, project, back, weights,
    sides, rims,
    out_modes, in_modes, out_coefs, in_coefs,
    sum_mine, sum_all, wall_out, wall_in,
    local_sem, halo_send, halo_recv, mode_send, mode_recv, coef_send, coef_recv,
    sum_send, sum_recv, wall_recv,
):
    nx, ny, nz = sizes
    x, y, z = (lax.axis_index(a) for a in GX)
    hi, core = (lax.axis_index(a) for a in GY)
    me = hi * 2 + core
    count = nx * ny * nz
    here = (x * ny + y) * nz + z

    def place(index):
        return {
            "gx_0": lax.div(index, ny * nz),
            "gx_1": lax.rem(lax.div(index, nz), ny),
            "gx_2": lax.rem(index, nz),
        }

    right = place(lax.rem(here + 1, count))
    left = place(lax.rem(here + count - 1, count))
    solvers = [{"gx_1": 1 - y, "gy_0": q // 2, "gy_1": q % 2} for q in range(4)]

    def stage_peer(stage, step):
        if stage == 0:
            index = lax.rem(z + step, nz)
            return index, {"gx_2": index}
        if stage == 1:
            index = lax.rem(x + step, nx)
            return index, {"gx_0": index}
        index = lax.rem(y * 4 + me + step, 4 * ny)
        return index, {
            "gx_1": lax.div(index, 4),
            "gy_0": lax.rem(lax.div(index, 2), 2),
            "gy_1": lax.rem(index, 2),
        }

    stage_me = (z, x, y * 4 + me)
    stage_size = (nz, nx, 4 * ny)
    peers = [stage_peer(k, n)[1] for k in range(3) for n in range(1, stage_size[k])]

    upper = lax.div(z, nz // 2)
    depth = upper * (nz - 1 - z) + (1 - upper) * z
    inner = z + 1 - 2 * upper
    outer = z - 1 + 2 * upper

    def at_plane(device, plane):
        return {**device, "gx_2": plane}

    barrier = pltpu.get_barrier_semaphore()
    met = [right, left, *peers]
    for device in met:
        pl.semaphore_signal(barrier, inc=1, device_id=device, device_id_type=MESH)
    for level, plane in ((0, inner), (1, outer)):
        @pl.when(depth == level)
        def _():
            for device in solvers:
                pl.semaphore_signal(
                    barrier, inc=1, device_id=at_plane(device, plane), device_id_type=MESH
                )

    state_loads = []
    for part, sem in ((pl.ds(0, STEP), 0), (pl.ds(STEP, MEMBERS - STEP), 8)):
        state_loads.append(
            pltpu.make_async_copy(state_hbm.at[part], state.at[part], local_sem.at[sem])
        )
    for load in state_loads:
        load.start()
    loads = [
        pltpu.make_async_copy(project_hbm, project, local_sem.at[1]),
        pltpu.make_async_copy(back_hbm, back, local_sem.at[2]),
        pltpu.make_async_copy(weights_hbm, weights, local_sem.at[7]),
    ]

    def inverse_load(k):
        part = pl.ds(k * UNROLL, UNROLL)
        return pltpu.make_async_copy(inverse_hbm.at[part], inverse.at[part], local_sem.at[3 + k])

    lane = lax.broadcasted_iota(jnp.int32, (1, PTS), 1)
    low_half = lane < LOCAL

    def halo_copies(step):
        rows = pl.ds(step * STEP, STEP)
        return [
            pltpu.make_async_remote_copy(
                sides.at[k, rows], rims.at[k, rows], halo_send.at[0], halo_recv.at[step],
                device_id=device, device_id_type=MESH,
            )
            for k, device in enumerate((right, left))
        ]

    def whole(buffer, sem):
        return pltpu.make_async_remote_copy(
            buffer, buffer, sem, sem, device_id=right, device_id_type=MESH
        )

    state_loads[0].wait()

    def pack(e):
        centre = state[e]
        top, low = centre[:, :32], centre[:, 32:]
        turned = pltpu.roll(low, LOCAL, 2)
        sides[0, e] = jnp.where(low_half, turned, top)
        sides[1, e] = jnp.where(low_half, top, turned)

    for k in range(STEP):
        pack(k)

    def squares(e, carry):
        values = state[e].reshape(FIELDS * LOCAL, PTS)
        total = jnp.sum(values * values, axis=0, keepdims=True)
        return jnp.where(lane == e, jnp.sum(total, axis=1, keepdims=True), carry)

    def sum_copy(stage, step):
        return pltpu.make_async_remote_copy(
            sum_mine.at[stage], sum_all.at[stage, stage_me[stage]],
            sum_send.at[stage], sum_recv.at[stage],
            device_id=stage_peer(stage, step)[1], device_id_type=MESH,
        )

    def sum_rest(stage, sem):
        return whole(sum_all.at[stage, pl.ds(0, stage_size[stage] - 1)], sem.at[stage])

    def sum_start(stage):
        for step in range(1, stage_size[stage]):
            sum_copy(stage, step).start()
        sum_all[stage, stage_me[stage]] = sum_mine[stage]

    def sum_end(stage):
        sum_rest(stage, sum_recv).wait_recv()
        total = sum_all[stage, 0]
        for k in range(1, stage_size[stage]):
            total = total + sum_all[stage, k]
        sum_mine[stage + 1] = total

    pl.semaphore_wait(barrier, len(met) + len(solvers) * (1 - lax.div(depth + 2, 4)))
    for copy in halo_copies(0):
        copy.start()
    state_loads[1].wait()
    for load in loads:
        load.start()
    for k in range(PIECES):
        inverse_load(k).start()
    sum_mine[0] = lax.fori_loop(0, MEMBERS, squares, jnp.zeros((1, PTS), F32))
    sum_start(0)

    def pack_and_send(step, carry):
        for k in range(STEP):
            pack(step * STEP + k)
        for copy in halo_copies(step):
            copy.start()
        return carry

    lax.fori_loop(1, STEPS, pack_and_send, 0)

    for load in loads:
        load.wait()

    def split_inverse(m, carry):
        high, low = split(inverse[m])
        inv_high[m] = high
        inv_low[m] = low
        return carry


    coupling_0 = jnp.where(low_half, TIME_STEP * CORIOLIS, TIME_STEP)
    coupling_1 = jnp.where(low_half, -TIME_STEP * CORIOLIS, -TIME_STEP * STRATIFICATION)
    coefficient = me * LOCAL + lax.rem(lane, LOCAL)
    interior = coefficient < 4 * LOCAL - 2

    def mode_copies(step):
        moved = lax.div(step, STEPS - STEP) * (1 - lax.div(depth + nz - 1, nz))
        target = step + moved * STEP
        rows = pl.ds(step * (STEP * BLOCK), STEP * BLOCK)
        target_rows = pl.ds(target * (STEP * BLOCK), STEP * BLOCK)
        return [
            pltpu.make_async_remote_copy(
                out_modes.at[q, rows], in_modes.at[me, target_rows],
                mode_send.at[0], mode_recv.at[lax.div(target, GROUP // STEP)],
                device_id=at_plane(solvers[q], z + moved * (1 - 2 * upper)), device_id_type=MESH,
            )
            for q in range(4)
        ]

    def project_member(e):
        centre = state[e]
        rim_left, rim_right = rims[0, e], rims[1, e]
        top = jnp.where(low_half, rim_right, rim_left)
        low = pltpu.roll(jnp.where(low_half, rim_left, rim_right), LOCAL, 2)
        rim = jnp.concatenate([top, low], axis=1)
        segment = jnp.concatenate(
            [centre.reshape(FIELDS * LOCAL, PTS), rim.reshape(FIELDS * LOCAL, PTS)], axis=1
        )
        high, low = split(segment)
        first = dot_t(project[...], high)
        second = dot_t(project[: 2 * MODES], low)
        both = first[: 2 * MODES] + (first[2 * MODES :] + second)
        a_0, a_1 = both[:MODES, :PTS], both[:MODES, PTS:]
        b_0, b_1 = both[MODES:, :PTS], both[MODES:, PTS:]
        rhs_0 = jnp.where(interior, a_0 + coupling_0 * b_1, 0.0)
        rhs_1 = jnp.where(interior, a_1 + coupling_1 * b_0, 0.0)
        for q in range(4):
            modes = slice(q * QUARTER, (q + 1) * QUARTER)
            base = pl.multiple_of(e * BLOCK, BLOCK)
            out_modes[q, pl.ds(base, QUARTER), :] = rhs_0[modes]
            out_modes[q, pl.ds(base + QUARTER, QUARTER), :] = rhs_1[modes]

    def project_step(step, carry):
        whole(rims.at[:, pl.ds(step * STEP, STEP)], halo_recv.at[step]).wait_recv()
        for k in range(STEP):
            project_member(step * STEP + k)
        for copy in mode_copies(step):
            copy.start()

        @pl.when(step < PIECES)
        def _():
            inverse_load(step).wait()
            lax.fori_loop(step * UNROLL, (step + 1) * UNROLL, split_inverse, 0)

        @pl.when(step == 2)
        def _():
            sum_end(0)
            sum_start(1)

        @pl.when(step == 4)
        def _():
            sum_end(1)
            sum_start(2)

        return carry

    lax.fori_loop(0, STEPS, project_step, 0)

    def back_to(slot, t):
        return at_plane(solvers[t], z + lax.div(slot, GROUPS) * (2 * upper - 1))

    def coef_copies(step):
        slot = lax.div(step, GROUP // STEP)
        moved = lax.div(slot, GROUPS)
        target = step - moved * (GROUP // STEP)
        rows = pl.ds(step * (STEP * BLOCK), STEP * BLOCK)
        target_rows = pl.ds(target * (STEP * BLOCK), STEP * BLOCK)
        return [
            pltpu.make_async_remote_copy(
                out_coefs.at[t, rows], in_coefs.at[me, target_rows],
                coef_send.at[0], coef_recv.at[target],
                device_id=back_to(slot, t), device_id_type=MESH,
            )
            for t in range(4)
        ]

    def wall_copies(slot):
        group = slot - lax.div(slot, GROUPS)
        return [
            pltpu.make_async_remote_copy(
                wall_out.at[slot], wall_in.at[me, group],
                coef_send.at[1], wall_recv.at[group],
                device_id=back_to(slot, t), device_id_type=MESH,
            )
            for t in range(4)
        ]

    def wall_sums(slot):
        rows = pl.ds(slot * (GROUP * BLOCK), GROUP * BLOCK)
        blocks = jnp.concatenate([out_coefs[t, rows, :] for t in range(4)], axis=1)
        high, low = split(blocks)
        first = dot_t(weights[...], high)
        second = dot_t(weights[:16], low)
        wall_out[slot] = (first[:16] + (first[16:] + second))[:2]

    def solved_here(slot):
        return (slot < GROUPS - 1) | ((slot == GROUPS - 1) & (depth > 0)) | ((slot == GROUPS) & (depth == 1))

    def turn(a):
        return pltpu.roll(a, LOCAL, 1)

    def solve_mode(base, m):
        rows = pl.ds(base + m, 2 * GROUP, stride=QUARTER)
        parts = [in_modes[s, rows, :] for s in range(4)]
        even, odd = [], []
        for s in (0, 2):
            first, second = parts[s], parts[s + 1]
            even.append(jnp.where(low_half, first, turn(second)))
            odd.append(jnp.where(low_half, turn(first), second))
        values = jnp.concatenate(
            [jnp.concatenate(even, axis=1), jnp.concatenate(odd, axis=1)], axis=0
        )
        high, low = split(values)
        count = 4 * GROUP
        first = dot_t(jnp.concatenate([high, low], axis=0), inv_high[m])
        second = dot_t(high, inv_low[m])
        solved = first[:count] + (first[count:] + second)
        even, odd = solved[: 2 * GROUP], solved[2 * GROUP :]
        for k in range(2):
            lanes = slice(k * PTS, (k + 1) * PTS)
            out_coefs[2 * k, rows, :] = jnp.where(low_half, even[:, lanes], turn(odd[:, lanes]))
            out_coefs[2 * k + 1, rows, :] = jnp.where(low_half, turn(even[:, lanes]), odd[:, lanes])

    def solve_group(group):
        rows = pl.ds(group * (GROUP * BLOCK), GROUP * BLOCK)
        whole(in_modes.at[:, rows], mode_recv.at[group]).wait_recv()
        base = group * (GROUP * BLOCK)

        def some_modes(k, carry):
            for u in range(UNROLL):
                solve_mode(base, k * UNROLL + u)
            return carry

        lax.fori_loop(0, QUARTER // UNROLL, some_modes, 0)
        for k in range(GROUP // STEP):
            for copy in coef_copies(group * (GROUP // STEP) + k):
                copy.start()
        wall_sums(group)
        for copy in wall_copies(group):
            copy.start()

    def solve_slot(turn, carry):
        slot = turn + lax.div(turn, GROUPS - 1) * (1 - 2 * lax.rem(turn, GROUPS - 1))

        @pl.when(solved_here(slot))
        def _():
            solve_group(slot)

        return carry

    lax.fori_loop(0, GROUPS + 1, solve_slot, 0)

    whole(sides, halo_send.at[0]).wait_send()
    whole(out_modes, mode_send.at[0]).wait_send()
    for stage in range(3):
        sum_rest(stage, sum_send).wait_send()

    grid = float(FIELDS * 4 * LOCAL * PTS * count)

    sum_end(2)

    def back_member(e):
        base = pl.multiple_of(e * BLOCK, BLOCK)
        turned = []
        for col in range(2):
            block = jnp.concatenate(
                [in_coefs[q, pl.ds(base + col * QUARTER, QUARTER), :] for q in range(4)], axis=0
            )
            turned.append(block.T)
        high, low = split(jnp.concatenate(turned, axis=0))
        values = dot(jnp.concatenate([high, low], axis=1), back[: 2 * MODES])
        values = values + dot(high, back[2 * MODES : 3 * MODES])
        total = jnp.sum(jnp.where(lane == e, sum_mine[3], 0.0), axis=1, keepdims=True)
        values = values * lax.rsqrt(total / grid + EPSILON)
        out_ref[e] = values.reshape(FIELDS, LOCAL, PTS)

    row = lax.broadcasted_iota(jnp.int32, (4 * GROUP, 2 * PTS), 0)
    lanes = lax.broadcasted_iota(jnp.int32, (4 * GROUP, 2 * PTS), 1)
    own = lax.div(lanes, QUARTER) == 2 * lax.div(row, 4) + lax.rem(row, 2)
    upper_wall = lax.rem(lax.div(row, 2), 2) == 0

    def wall_group(group):
        whole(wall_in.at[:, group], wall_recv.at[group]).wait_recv()
        parts = []
        for q in range(4):
            both = wall_in[q, group]
            parts.append(jnp.where(own, jnp.where(upper_wall, both[:1], both[1:]), 0.0))
        high, low = split(jnp.concatenate(parts, axis=1))
        table = back[3 * MODES : 11 * MODES]
        first = dot(jnp.concatenate([high, low], axis=0), table)
        count = 4 * GROUP
        values = first[:count] + (first[count:] + dot(high, back[11 * MODES :]))
        member = group * GROUP + lax.div(row[:, :PTS], 4)
        total = jnp.sum(jnp.where(lane == member, sum_mine[3], 0.0), axis=1, keepdims=True)
        values = values * lax.rsqrt(total / grid + EPSILON)
        for e in range(GROUP):
            for w in range(2):
                wall_ref[group * GROUP + e, w] = values[4 * e + 2 * w : 4 * e + 2 * w + 2]

    def back_step(step, carry):
        rows = pl.ds(step * (STEP * BLOCK), STEP * BLOCK)
        whole(in_coefs.at[:, rows], coef_recv.at[step]).wait_recv()
        for k in range(STEP):
            back_member(step * STEP + k)

        @pl.when(lax.rem(step, 2) == 1)
        def _():
            wall_group(lax.div(step, 2))

        return carry

    lax.fori_loop(0, STEPS, back_step, 0)

    for held, here_now in (
        (GROUPS - 1, depth == 0), (GROUPS + 1, depth == 1), (GROUPS, depth > 1)
    ):
        @pl.when(here_now)
        def _():
            whole(out_coefs.at[:, pl.ds(0, held * GROUP * BLOCK)], coef_send.at[0]).wait_send()
            whole(wall_in.at[:, pl.ds(0, held)], coef_send.at[1]).wait_send()


def per_device(sizes, state, inverse):
    both, back = window_tables(PTS + 2 * HALO, HALO, PTS, MODES)
    project = jnp.asarray(np.concatenate(split_table(both), axis=0))
    high, low = split_table(back)

    def tiled(table):
        quarters = table.reshape(4, QUARTER, PTS)
        return np.concatenate([q for part in quarters for q in [part] * (2 * GROUP)], axis=0)

    back = jnp.asarray(np.concatenate([high, high, low, tiled(high), tiled(low)], axis=0))
    k = np.arange(4 * LOCAL, dtype=np.float64)
    curvature = k * k / (4 * LOCAL) ** 2
    walls = np.zeros((16, 4, 2, LOCAL))
    walls[0, :, 0] = curvature.reshape(4, LOCAL)
    walls[1, :, 0] = np.where(k % 2 == 0, -curvature, curvature).reshape(4, LOCAL)
    weights = jnp.asarray(np.concatenate(split_table(walls.reshape(16, 8 * LOCAL)), axis=0))
    exchange = (4, MEMBERS * BLOCK, PTS)
    larger = (4, (MEMBERS + GROUP) * BLOCK, PTS)
    rim = (2, MEMBERS, FIELDS, 32, PTS)
    vmem = pltpu.VMEM
    dma = pltpu.SemaphoreType.DMA
    updated, wall = pl.pallas_call(
        functools.partial(kernel, sizes),
        out_shape=(
            pltpu.VMEM(state.shape, F32),
            pltpu.VMEM((MEMBERS, 2, 2, PTS), F32),
        ),
        in_specs=[pl.BlockSpec(memory_space=pl.ANY)] * 5,
        out_specs=(
            pl.BlockSpec(memory_space=pltpu.VMEM),
            pl.BlockSpec(memory_space=pltpu.VMEM),
        ),
        scratch_shapes=[
            vmem(state.shape, F32),
            vmem(inverse.shape, F32),
            vmem(inverse.shape, BF16),
            vmem(inverse.shape, BF16),
            vmem(project.shape, BF16),
            vmem(back.shape, BF16),
            vmem(weights.shape, BF16),
            *[vmem(rim, F32)] * 2,
            vmem(exchange, F32),
            vmem(larger, F32),
            vmem(larger, F32),
            vmem(exchange, F32),
            vmem((4, 1, PTS), F32),
            vmem((3, 8, 1, PTS), F32),
            vmem((GROUPS + 1, 2, 2 * PTS), F32),
            vmem((4, GROUPS + 1, 2, 2 * PTS), F32),
            dma((9,)),
            dma((1,)),
            dma((STEPS,)),
            dma((1,)),
            dma((GROUPS + 1,)),
            dma((2,)),
            dma((STEPS,)),
            dma((3,)),
            dma((3,)),
            dma((GROUPS,)),
        ],
        compiler_params=pltpu.CompilerParams(
            collective_id=0, has_side_effects=True, vmem_limit_bytes=56 * 1024 * 1024
        ),
        name="step",
    )(state, inverse, project, back, weights)
    return updated, wall


def solution(mesh):
    torus = Mesh(mesh.devices.reshape(4, 2, 8, 2, 2), AXES)
    return jax.shard_map(
        functools.partial(per_device, (4, 2, 8)),
        mesh=torus,
        in_specs=(P(None, None, GY, GX), P(GY, None, None)),
        out_specs=(P(None, None, GY, GX), P(None, None, None, GX)),
        check_vma=False,
    )
```

```python
import functools

import jax
import jax.numpy as jnp
import numpy as np
from jax import lax
from jax.experimental import pallas as pl
from jax.experimental.pallas import tpu as pltpu
from jax.sharding import Mesh
from jax.sharding import PartitionSpec as P

MODES = 128
HALO = 64
AXES = ("gx_0", "gx_1", "gx_2", "gy_0", "gy_1")
GX = ("gx_0", "gx_1", "gx_2")
GY = ("gy_0", "gy_1")
EPSILON = 1e-06
TIME_STEP = 0.5
MEAN_FLOW = 0.8
CORIOLIS = 0.6
STRATIFICATION = 0.9
F32 = jnp.float32
BF16 = jnp.bfloat16
MESH = pl.DeviceIdType.MESH

MEMBERS = 12
FIELDS = 4
LOCAL = 64
PTS = 128
QUARTER = 32
BLOCK = 2 * QUARTER
STEP = 2
STEPS = MEMBERS // STEP
GROUP = 2
GROUPS = MEMBERS // GROUP
UNROLL = 32
SPAN = 2 * GROUP * QUARTER
MOVED = (3, 1)
FOREIGN = 3
SLOTS = GROUPS + FOREIGN
PIECES = 4
PIECE = QUARTER // PIECES


def window_tables(window, rim, points, modes):
    pos = np.arange(window)
    mode = np.arange(modes)
    half = modes // 2
    cosine = mode <= half
    wave = np.where(cosine, mode, mode - half)
    phase = 2.0 * np.pi * (pos[:, None] * wave[None, :] % window) / window
    norm = np.where(wave == 0, np.sqrt(1.0 / window), np.sqrt(2.0 / window))
    basis = np.where(cosine[None, :], np.cos(phase), np.sin(phase)) * norm[None, :]
    kappa = 2.0 * np.pi * wave / window
    paired = wave[:, None] == wave[None, :]
    to_sine = cosine[:, None] & ~cosine[None, :] & paired
    to_cosine = ~cosine[:, None] & cosine[None, :] & paired
    derivative = np.where(to_sine, -kappa[:, None], 0.0) + np.where(to_cosine, kappa[:, None], 0.0)
    taper = 0.25 + 0.75 * np.sin(np.pi * (pos + 0.5) / window) ** 2
    plain = basis * taper[:, None]
    slope = (basis @ derivative) * taper[:, None]
    both = np.concatenate([plain - TIME_STEP * MEAN_FLOW * slope, plain], axis=1).T
    order = np.concatenate([np.arange(rim, window), np.arange(rim)])
    back = (basis[rim : rim + points] / taper[rim : rim + points, None]).T
    return both[:, order], back


def split_table(table):
    high = table.astype(BF16)
    low = (table - high.astype(np.float64)).astype(BF16)
    return high, low


def split(a):
    high = a.astype(BF16)
    low = (a - high.astype(F32)).astype(BF16)
    return high, low


def dot_t(a, b):
    return lax.dot_general(a, b, (((1,), (1,)), ((), ())), preferred_element_type=F32)


def dot(a, b):
    return lax.dot_general(a, b, (((1,), (0,)), ((), ())), preferred_element_type=F32)


def kernel(
    sizes,
    state_hbm, inverse_hbm, project_hbm, back_hbm, weights_hbm, out_ref, wall_ref,
    state, inverse, inv_high, inv_low, project, back, weights,
    sides, rims,
    out_modes, in_modes, out_coefs, in_coefs,
    sum_mine, sum_all, wall_out, wall_in,
    local_sem, halo_send, halo_recv, mode_send, mode_recv, coef_send, coef_recv,
    sum_send, sum_recv, wall_recv,
):
    nx, ny, nz = sizes
    x, y, z = (lax.axis_index(a) for a in GX)
    hi, core = (lax.axis_index(a) for a in GY)
    me = hi * 2 + core
    count = nx * ny * nz
    here = (x * ny + y) * nz + z

    def place(index):
        return {
            "gx_0": lax.div(index, ny * nz),
            "gx_1": lax.rem(lax.div(index, nz), ny),
            "gx_2": lax.rem(index, nz),
        }

    right = place(lax.rem(here + 1, count))
    left = place(lax.rem(here + count - 1, count))
    solvers = [{"gx_1": 1 - y, "gy_0": q // 2, "gy_1": q % 2} for q in range(4)]

    def stage_peer(stage, step):
        if stage == 0:
            index = lax.rem(z + step, nz)
            return index, {"gx_2": index}
        if stage == 1:
            index = lax.rem(x + step, nx)
            return index, {"gx_0": index}
        index = lax.rem(y * 4 + me + step, 4 * ny)
        return index, {
            "gx_1": lax.div(index, 4),
            "gy_0": lax.rem(lax.div(index, 2), 2),
            "gy_1": lax.rem(index, 2),
        }

    stage_me = (z, x, y * 4 + me)
    stage_size = (nz, nx, 4 * ny)
    peers = [stage_peer(k, n)[1] for k in range(3) for n in range(1, stage_size[k])]

    upper = lax.div(z, nz // 2)
    depth = upper * (nz - 1 - z) + (1 - upper) * z
    from_top = nz // 2 - 1 - depth
    at_0 = lax.div(from_top, 3)
    at_1 = lax.div(from_top, 2) - at_0
    at_2 = from_top - 2 * lax.div(from_top, 2) - at_0
    leaving = MOVED[0] * at_0 + MOVED[1] * at_1
    coming = MOVED[0] * at_1 + MOVED[1] * at_2
    inner = z + 1 - 2 * upper
    outer = z - 1 + 2 * upper

    def at_plane(device, plane):
        return {**device, "gx_2": plane}

    barrier = pltpu.get_barrier_semaphore()
    met = [right, left, *peers]
    for device in met:
        pl.semaphore_signal(barrier, inc=1, device_id=device, device_id_type=MESH)
    for near_end, plane in ((depth < 2, inner), ((depth == 1) | (depth == 2), outer)):
        @pl.when(near_end)
        def _():
            for device in solvers:
                pl.semaphore_signal(
                    barrier, inc=1, device_id=at_plane(device, plane), device_id_type=MESH
                )

    state_loads = []
    for part, sem in ((pl.ds(0, STEP), 0), (pl.ds(STEP, MEMBERS - STEP), 8)):
        state_loads.append(
            pltpu.make_async_copy(state_hbm.at[part], state.at[part], local_sem.at[sem])
        )
    for load in state_loads:
        load.start()
    loads = [
        pltpu.make_async_copy(project_hbm, project, local_sem.at[1]),
        pltpu.make_async_copy(back_hbm, back, local_sem.at[2]),
        pltpu.make_async_copy(weights_hbm, weights, local_sem.at[7]),
    ]

    def inverse_load(k):
        part = pl.ds(k * PIECE, PIECE)
        return pltpu.make_async_copy(inverse_hbm.at[part], inverse.at[part], local_sem.at[3 + k])

    lane = lax.broadcasted_iota(jnp.int32, (1, PTS), 1)
    low_half = lane < LOCAL

    def halo_copies(step):
        rows = pl.ds(step * STEP, STEP)
        return [
            pltpu.make_async_remote_copy(
                sides.at[k, rows], rims.at[k, rows], halo_send.at[0], halo_recv.at[step],
                device_id=device, device_id_type=MESH,
            )
            for k, device in enumerate((right, left))
        ]

    def whole(buffer, sem):
        return pltpu.make_async_remote_copy(
            buffer, buffer, sem, sem, device_id=right, device_id_type=MESH
        )

    state_loads[0].wait()

    def pack(e):
        centre = state[e]
        top, low = centre[:, :32], centre[:, 32:]
        turned = pltpu.roll(low, LOCAL, 2)
        sides[0, e] = jnp.where(low_half, turned, top)
        sides[1, e] = jnp.where(low_half, top, turned)

    for k in range(STEP):
        pack(k)

    def squares(e, carry):
        values = state[e].reshape(FIELDS * LOCAL, PTS)
        total = jnp.sum(values * values, axis=0, keepdims=True)
        return jnp.where(lane == e, jnp.sum(total, axis=1, keepdims=True), carry)

    def sum_copy(stage, step):
        return pltpu.make_async_remote_copy(
            sum_mine.at[stage], sum_all.at[stage, stage_me[stage]],
            sum_send.at[stage], sum_recv.at[stage],
            device_id=stage_peer(stage, step)[1], device_id_type=MESH,
        )

    def sum_rest(stage, sem):
        return whole(sum_all.at[stage, pl.ds(0, stage_size[stage] - 1)], sem.at[stage])

    def sum_start(stage):
        for step in range(1, stage_size[stage]):
            sum_copy(stage, step).start()
        sum_all[stage, stage_me[stage]] = sum_mine[stage]

    def sum_end(stage):
        sum_rest(stage, sum_recv).wait_recv()
        total = sum_all[stage, 0]
        for k in range(1, stage_size[stage]):
            total = total + sum_all[stage, k]
        sum_mine[stage + 1] = total

    pl.semaphore_wait(barrier, len(met) + len(solvers) * (at_0 + 2 * at_1 + at_2))
    for copy in halo_copies(0):
        copy.start()
    state_loads[1].wait()
    for load in loads:
        load.start()
    for k in range(PIECES):
        inverse_load(k).start()
    sum_mine[0] = lax.fori_loop(0, MEMBERS, squares, jnp.zeros((1, PTS), F32))
    sum_start(0)

    def pack_and_send(step, carry):
        for k in range(STEP):
            pack(step * STEP + k)
        for copy in halo_copies(step):
            copy.start()
        return carry

    lax.fori_loop(1, STEPS, pack_and_send, 0)

    for load in loads:
        load.wait()

    def split_inverse(m, carry):
        high, low = split(inverse[m])
        inv_high[m] = high
        inv_low[m] = low
        return carry


    coupling_0 = jnp.where(low_half, TIME_STEP * CORIOLIS, TIME_STEP)
    coupling_1 = jnp.where(low_half, -TIME_STEP * CORIOLIS, -TIME_STEP * STRATIFICATION)
    coefficient = me * LOCAL + lax.rem(lane, LOCAL)
    interior = coefficient < 4 * LOCAL - 2

    def mode_copies(step):
        moved = lax.div(step + leaving, GROUPS)
        target = step + moved * FOREIGN
        rows = pl.ds(step * (STEP * BLOCK), STEP * BLOCK)
        target_rows = pl.ds(target * (STEP * BLOCK), STEP * BLOCK)
        return [
            pltpu.make_async_remote_copy(
                out_modes.at[q, rows], in_modes.at[me, target_rows],
                mode_send.at[0], mode_recv.at[target],
                device_id=at_plane(solvers[q], z + moved * (1 - 2 * upper)), device_id_type=MESH,
            )
            for q in range(4)
        ]

    def project_member(e):
        centre = state[e]
        rim_left, rim_right = rims[0, e], rims[1, e]
        top = jnp.where(low_half, rim_right, rim_left)
        low = pltpu.roll(jnp.where(low_half, rim_left, rim_right), LOCAL, 2)
        rim = jnp.concatenate([top, low], axis=1)
        segment = jnp.concatenate(
            [centre.reshape(FIELDS * LOCAL, PTS), rim.reshape(FIELDS * LOCAL, PTS)], axis=1
        )
        high, low = split(segment)
        first = dot_t(project[...], high)
        second = dot_t(project[: 2 * MODES], low)
        both = first[: 2 * MODES] + (first[2 * MODES :] + second)
        a_0, a_1 = both[:MODES, :PTS], both[:MODES, PTS:]
        b_0, b_1 = both[MODES:, :PTS], both[MODES:, PTS:]
        rhs_0 = jnp.where(interior, a_0 + coupling_0 * b_1, 0.0)
        rhs_1 = jnp.where(interior, a_1 + coupling_1 * b_0, 0.0)
        for q in range(4):
            modes = slice(q * QUARTER, (q + 1) * QUARTER)
            base = pl.multiple_of(e * BLOCK, BLOCK)
            out_modes[q, pl.ds(base, QUARTER), :] = rhs_0[modes]
            out_modes[q, pl.ds(base + QUARTER, QUARTER), :] = rhs_1[modes]

    def project_step(step, carry):
        whole(rims.at[:, pl.ds(step * STEP, STEP)], halo_recv.at[step]).wait_recv()
        for k in range(STEP):
            project_member(step * STEP + k)
        for copy in mode_copies(step):
            copy.start()

        @pl.when(step < PIECES)
        def _():
            inverse_load(step).wait()
            lax.fori_loop(step * PIECE, (step + 1) * PIECE, split_inverse, 0)

        @pl.when(step == 2)
        def _():
            sum_end(0)
            sum_start(1)

        @pl.when(step == 4)
        def _():
            sum_end(1)
            sum_start(2)

        return carry

    lax.fori_loop(0, STEPS, project_step, 0)

    def back_to(slot, t):
        return at_plane(solvers[t], z + lax.div(slot, GROUPS) * (2 * upper - 1))

    def coef_copies(slot):
        target = slot - lax.div(slot, GROUPS) * FOREIGN
        rows = pl.ds(slot * (STEP * BLOCK), STEP * BLOCK)
        target_rows = pl.ds(target * (STEP * BLOCK), STEP * BLOCK)
        return [
            pltpu.make_async_remote_copy(
                out_coefs.at[t, rows], in_coefs.at[me, target_rows],
                coef_send.at[0], coef_recv.at[target],
                device_id=back_to(slot, t), device_id_type=MESH,
            )
            for t in range(4)
        ]

    def wall_copies(slot):
        group = slot - lax.div(slot, GROUPS) * FOREIGN
        return [
            pltpu.make_async_remote_copy(
                wall_out.at[slot], wall_in.at[me, group],
                coef_send.at[1], wall_recv.at[group],
                device_id=back_to(slot, t), device_id_type=MESH,
            )
            for t in range(4)
        ]

    def wall_sums(slot):
        rows = pl.ds(slot * (GROUP * BLOCK), GROUP * BLOCK)
        blocks = jnp.concatenate([out_coefs[t, rows, :] for t in range(4)], axis=1)
        high, low = split(blocks)
        first = dot_t(weights[...], high)
        second = dot_t(weights[:16], low)
        wall_out[slot] = (first[:16] + (first[16:] + second))[:2]

    def solved_here(slot):
        own = (slot < GROUPS) & (slot < GROUPS - leaving)
        return own | ((slot >= GROUPS) & (slot >= SLOTS - coming))

    def turn(a):
        return pltpu.roll(a, LOCAL, 1)

    def solve_mode(base, m):
        rows = pl.ds(base + m, 2 * GROUP, stride=QUARTER)
        parts = [in_modes[s, rows, :] for s in range(4)]
        even, odd = [], []
        for s in (0, 2):
            first, second = parts[s], parts[s + 1]
            even.append(jnp.where(low_half, first, turn(second)))
            odd.append(jnp.where(low_half, turn(first), second))
        values = jnp.concatenate(
            [jnp.concatenate(even, axis=1), jnp.concatenate(odd, axis=1)], axis=0
        )
        high, low = split(values)
        count = 4 * GROUP
        first = dot_t(jnp.concatenate([high, low], axis=0), inv_high[m])
        second = dot_t(high, inv_low[m])
        solved = first[:count] + (first[count:] + second)
        even, odd = solved[: 2 * GROUP], solved[2 * GROUP :]
        for k in range(2):
            lanes = slice(k * PTS, (k + 1) * PTS)
            out_coefs[2 * k, rows, :] = jnp.where(low_half, even[:, lanes], turn(odd[:, lanes]))
            out_coefs[2 * k + 1, rows, :] = jnp.where(low_half, turn(even[:, lanes]), odd[:, lanes])

    def solve_group(group):
        rows = pl.ds(group * (GROUP * BLOCK), GROUP * BLOCK)
        whole(in_modes.at[:, rows], mode_recv.at[group]).wait_recv()
        base = group * (GROUP * BLOCK)

        def some_modes(k, carry):
            for u in range(UNROLL):
                solve_mode(base, k * UNROLL + u)
            return carry

        lax.fori_loop(0, QUARTER // UNROLL, some_modes, 0)
        for copy in coef_copies(group):
            copy.start()
        wall_sums(group)
        for copy in wall_copies(group):
            copy.start()

    def solve_slot(turn, carry):
        late = lax.div(turn + FOREIGN, GROUPS)
        later = lax.div(turn + FOREIGN, 2) + FOREIGN * (1 - lax.rem(turn + FOREIGN, 2))
        slot = (1 - late) * turn + late * later

        @pl.when(solved_here(slot))
        def _():
            solve_group(slot)

        return carry

    lax.fori_loop(0, SLOTS, solve_slot, 0)

    whole(sides, halo_send.at[0]).wait_send()
    whole(out_modes, mode_send.at[0]).wait_send()
    for stage in range(3):
        sum_rest(stage, sum_send).wait_send()

    grid = float(FIELDS * 4 * LOCAL * PTS * count)

    sum_end(2)

    def back_member(e):
        base = pl.multiple_of(e * BLOCK, BLOCK)
        turned = []
        for col in range(2):
            block = jnp.concatenate(
                [in_coefs[q, pl.ds(base + col * QUARTER, QUARTER), :] for q in range(4)], axis=0
            )
            turned.append(block.T)
        high, low = split(jnp.concatenate(turned, axis=0))
        values = dot(jnp.concatenate([high, low], axis=1), back[: 2 * MODES])
        values = values + dot(high, back[2 * MODES : 3 * MODES])
        total = jnp.sum(jnp.where(lane == e, sum_mine[3], 0.0), axis=1, keepdims=True)
        values = values * lax.rsqrt(total / grid + EPSILON)
        out_ref[e] = values.reshape(FIELDS, LOCAL, PTS)

    row = lax.broadcasted_iota(jnp.int32, (4 * GROUP, SPAN), 0)
    lanes = lax.broadcasted_iota(jnp.int32, (4 * GROUP, SPAN), 1)
    own = lax.div(lanes, QUARTER) == 2 * lax.div(row, 4) + lax.rem(row, 2)
    upper_wall = lax.rem(lax.div(row, 2), 2) == 0

    def wall_group(group):
        whole(wall_in.at[:, group], wall_recv.at[group]).wait_recv()
        parts = []
        for q in range(4):
            both = wall_in[q, group]
            parts.append(jnp.where(own, jnp.where(upper_wall, both[:1], both[1:]), 0.0))
        high, low = split(jnp.concatenate(parts, axis=1))
        table = back[3 * MODES : 3 * MODES + 4 * SPAN]
        first = dot(jnp.concatenate([high, low], axis=0), table)
        count = 4 * GROUP
        values = first[:count] + (first[count:] + dot(high, back[3 * MODES + 4 * SPAN :]))
        member = group * GROUP + lax.div(row[:, :PTS], 4)
        total = jnp.sum(jnp.where(lane == member, sum_mine[3], 0.0), axis=1, keepdims=True)
        values = values * lax.rsqrt(total / grid + EPSILON)
        for e in range(GROUP):
            for w in range(2):
                wall_ref[group * GROUP + e, w] = values[4 * e + 2 * w : 4 * e + 2 * w + 2]

    def back_step(step, carry):
        rows = pl.ds(step * (STEP * BLOCK), STEP * BLOCK)
        whole(in_coefs.at[:, rows], coef_recv.at[step]).wait_recv()
        for k in range(STEP):
            back_member(step * STEP + k)

        wall_group(step)
        return carry

    lax.fori_loop(0, STEPS, back_step, 0)

    for held, here_now in (
        (GROUPS - MOVED[0], depth == 0), (GROUPS - MOVED[1] + MOVED[0], depth == 1),
        (GROUPS + MOVED[1], depth == 2), (GROUPS, depth > 2),
    ):
        @pl.when(here_now)
        def _():
            whole(out_coefs.at[:, pl.ds(0, held * GROUP * BLOCK)], coef_send.at[0]).wait_send()
            whole(wall_in.at[:, pl.ds(0, held)], coef_send.at[1]).wait_send()


def per_device(sizes, state, inverse):
    both, back = window_tables(PTS + 2 * HALO, HALO, PTS, MODES)
    project = jnp.asarray(np.concatenate(split_table(both), axis=0))
    high, low = split_table(back)

    def tiled(table):
        quarters = table.reshape(4, QUARTER, PTS)
        return np.concatenate([q for part in quarters for q in [part] * (2 * GROUP)], axis=0)

    back = jnp.asarray(np.concatenate([high, high, low, tiled(high), tiled(low)], axis=0))
    k = np.arange(4 * LOCAL, dtype=np.float64)
    curvature = k * k / (4 * LOCAL) ** 2
    walls = np.zeros((16, 4, 2, LOCAL))
    walls[0, :, 0] = curvature.reshape(4, LOCAL)
    walls[1, :, 0] = np.where(k % 2 == 0, -curvature, curvature).reshape(4, LOCAL)
    weights = jnp.asarray(np.concatenate(split_table(walls.reshape(16, 8 * LOCAL)), axis=0))
    exchange = (4, MEMBERS * BLOCK, PTS)
    larger = (4, SLOTS * GROUP * BLOCK, PTS)
    rim = (2, MEMBERS, FIELDS, 32, PTS)
    vmem = pltpu.VMEM
    dma = pltpu.SemaphoreType.DMA
    updated, wall = pl.pallas_call(
        functools.partial(kernel, sizes),
        out_shape=(
            pltpu.VMEM(state.shape, F32),
            pltpu.VMEM((MEMBERS, 2, 2, PTS), F32),
        ),
        in_specs=[pl.BlockSpec(memory_space=pl.ANY)] * 5,
        out_specs=(
            pl.BlockSpec(memory_space=pltpu.VMEM),
            pl.BlockSpec(memory_space=pltpu.VMEM),
        ),
        scratch_shapes=[
            vmem(state.shape, F32),
            vmem(inverse.shape, F32),
            vmem(inverse.shape, BF16),
            vmem(inverse.shape, BF16),
            vmem(project.shape, BF16),
            vmem(back.shape, BF16),
            vmem(weights.shape, BF16),
            *[vmem(rim, F32)] * 2,
            vmem(exchange, F32),
            vmem(larger, F32),
            vmem(larger, F32),
            vmem(exchange, F32),
            vmem((4, 1, PTS), F32),
            vmem((3, 8, 1, PTS), F32),
            vmem((SLOTS, 2, SPAN), F32),
            vmem((4, SLOTS, 2, SPAN), F32),
            dma((9,)),
            dma((1,)),
            dma((STEPS,)),
            dma((1,)),
            dma((SLOTS,)),
            dma((2,)),
            dma((STEPS,)),
            dma((3,)),
            dma((3,)),
            dma((GROUPS,)),
        ],
        compiler_params=pltpu.CompilerParams(
            collective_id=0, has_side_effects=True, vmem_limit_bytes=56 * 1024 * 1024
        ),
        name="step",
    )(state, inverse, project, back, weights)
    return updated, wall


def solution(mesh):
    torus = Mesh(mesh.devices.reshape(4, 2, 8, 2, 2), AXES)
    return jax.shard_map(
        functools.partial(per_device, (4, 2, 8)),
        mesh=torus,
        in_specs=(P(None, None, GY, GX), P(GY, None, None)),
        out_specs=(P(None, None, GY, GX), P(None, None, None, GX)),
        check_vma=False,
    )
```

```python
import functools

import jax
import jax.numpy as jnp
import numpy as np
from jax import lax
from jax.experimental import pallas as pl
from jax.experimental.pallas import tpu as pltpu
from jax.sharding import Mesh
from jax.sharding import PartitionSpec as P

MODES = 128
HALO = 64
AXES = ("gx_0", "gx_1", "gx_2", "gy_0", "gy_1")
GX = ("gx_0", "gx_1", "gx_2")
GY = ("gy_0", "gy_1")
EPSILON = 1e-06
TIME_STEP = 0.5
MEAN_FLOW = 0.8
CORIOLIS = 0.6
STRATIFICATION = 0.9
F32 = jnp.float32
BF16 = jnp.bfloat16
MESH = pl.DeviceIdType.MESH

MEMBERS = 12
FIELDS = 4
LOCAL = 64
PTS = 128
QUARTER = 32
BLOCK = 2 * QUARTER
STEP = 2
STEPS = MEMBERS // STEP
GROUP = 2
GROUPS = MEMBERS // GROUP
UNROLL = 32
SPAN = 2 * GROUP * QUARTER
MOVED = (3, 1)
FOREIGN = 3
SLOTS = GROUPS + FOREIGN
PIECES = 4
PIECE = QUARTER // PIECES


def window_tables(window, rim, points, modes):
    pos = np.arange(window)
    mode = np.arange(modes)
    half = modes // 2
    cosine = mode <= half
    wave = np.where(cosine, mode, mode - half)
    phase = 2.0 * np.pi * (pos[:, None] * wave[None, :] % window) / window
    norm = np.where(wave == 0, np.sqrt(1.0 / window), np.sqrt(2.0 / window))
    basis = np.where(cosine[None, :], np.cos(phase), np.sin(phase)) * norm[None, :]
    kappa = 2.0 * np.pi * wave / window
    paired = wave[:, None] == wave[None, :]
    to_sine = cosine[:, None] & ~cosine[None, :] & paired
    to_cosine = ~cosine[:, None] & cosine[None, :] & paired
    derivative = np.where(to_sine, -kappa[:, None], 0.0) + np.where(to_cosine, kappa[:, None], 0.0)
    taper = 0.25 + 0.75 * np.sin(np.pi * (pos + 0.5) / window) ** 2
    plain = basis * taper[:, None]
    slope = (basis @ derivative) * taper[:, None]
    both = np.concatenate([plain - TIME_STEP * MEAN_FLOW * slope, plain], axis=1).T
    order = np.concatenate([np.arange(rim, window), np.arange(rim)])
    back = (basis[rim : rim + points] / taper[rim : rim + points, None]).T
    return both[:, order], back


def split_table(table):
    high = table.astype(BF16)
    low = (table - high.astype(np.float64)).astype(BF16)
    return high, low


def split(a):
    high = a.astype(BF16)
    low = (a - high.astype(F32)).astype(BF16)
    return high, low


def dot_t(a, b):
    return lax.dot_general(a, b, (((1,), (1,)), ((), ())), preferred_element_type=F32)


def dot(a, b):
    return lax.dot_general(a, b, (((1,), (0,)), ((), ())), preferred_element_type=F32)


def kernel(
    sizes,
    state_hbm, inverse_hbm, project_hbm, back_hbm, weights_hbm, out_ref, wall_ref,
    state, inverse, inv_high, inv_low, project, back, weights,
    sides, rims,
    out_modes, in_modes, out_coefs, in_coefs,
    sum_mine, sum_all, wall_out, wall_in,
    local_sem, halo_send, halo_recv, mode_send, mode_recv, coef_send, coef_recv,
    sum_send, sum_recv, wall_recv,
):
    nx, ny, nz = sizes
    x, y, z = (lax.axis_index(a) for a in GX)
    hi, core = (lax.axis_index(a) for a in GY)
    me = hi * 2 + core
    count = nx * ny * nz
    here = (x * ny + y) * nz + z

    def place(index):
        return {
            "gx_0": lax.div(index, ny * nz),
            "gx_1": lax.rem(lax.div(index, nz), ny),
            "gx_2": lax.rem(index, nz),
        }

    right = place(lax.rem(here + 1, count))
    left = place(lax.rem(here + count - 1, count))
    solvers = [{"gx_1": 1 - y, "gy_0": q // 2, "gy_1": q % 2} for q in range(4)]

    def stage_peer(stage, step):
        if stage == 0:
            index = lax.rem(z + step, nz)
            return index, {"gx_2": index}
        if stage == 1:
            index = lax.rem(x + step, nx)
            return index, {"gx_0": index}
        index = lax.rem(y * 4 + me + step, 4 * ny)
        return index, {
            "gx_1": lax.div(index, 4),
            "gy_0": lax.rem(lax.div(index, 2), 2),
            "gy_1": lax.rem(index, 2),
        }

    stage_me = (z, x, y * 4 + me)
    stage_size = (nz, nx, 4 * ny)
    peers = [stage_peer(k, n)[1] for k in range(3) for n in range(1, stage_size[k])]

    upper = lax.div(z, nz // 2)
    depth = upper * (nz - 1 - z) + (1 - upper) * z
    from_top = nz // 2 - 1 - depth
    at_0 = lax.div(from_top, 3)
    at_1 = lax.div(from_top, 2) - at_0
    at_2 = from_top - 2 * lax.div(from_top, 2) - at_0
    leaving = MOVED[0] * at_0 + MOVED[1] * at_1
    coming = MOVED[0] * at_1 + MOVED[1] * at_2
    inner = z + 1 - 2 * upper
    outer = z - 1 + 2 * upper

    def at_plane(device, plane):
        return {**device, "gx_2": plane}

    barrier = pltpu.get_barrier_semaphore()
    met = [right, left, *peers]
    for device in met:
        pl.semaphore_signal(barrier, inc=1, device_id=device, device_id_type=MESH)
    for near_end, plane in ((depth < 2, inner), ((depth == 1) | (depth == 2), outer)):
        @pl.when(near_end)
        def _():
            for device in solvers:
                pl.semaphore_signal(
                    barrier, inc=1, device_id=at_plane(device, plane), device_id_type=MESH
                )

    state_loads = []
    for part, sem in ((pl.ds(0, STEP), 0), (pl.ds(STEP, MEMBERS - STEP), 8)):
        state_loads.append(
            pltpu.make_async_copy(state_hbm.at[part], state.at[part], local_sem.at[sem])
        )
    for load in state_loads:
        load.start()
    loads = [
        pltpu.make_async_copy(project_hbm, project, local_sem.at[1]),
        pltpu.make_async_copy(back_hbm, back, local_sem.at[2]),
        pltpu.make_async_copy(weights_hbm, weights, local_sem.at[7]),
    ]

    def inverse_load(k):
        part = pl.ds(k * PIECE, PIECE)
        return pltpu.make_async_copy(inverse_hbm.at[part], inverse.at[part], local_sem.at[3 + k])

    lane = lax.broadcasted_iota(jnp.int32, (1, PTS), 1)
    low_half = lane < LOCAL

    def halo_copies(step):
        rows = pl.ds(step * STEP, STEP)
        return [
            pltpu.make_async_remote_copy(
                sides.at[k, rows], rims.at[k, rows], halo_send.at[0], halo_recv.at[step],
                device_id=device, device_id_type=MESH,
            )
            for k, device in enumerate((right, left))
        ]

    def whole(buffer, sem):
        return pltpu.make_async_remote_copy(
            buffer, buffer, sem, sem, device_id=right, device_id_type=MESH
        )

    state_loads[0].wait()

    def pack(e):
        centre = state[e]
        top, low = centre[:, :32], centre[:, 32:]
        turned = pltpu.roll(low, LOCAL, 2)
        sides[0, e] = jnp.where(low_half, turned, top)
        sides[1, e] = jnp.where(low_half, top, turned)

    for k in range(STEP):
        pack(k)

    def squares(e, carry):
        values = state[e].reshape(FIELDS * LOCAL, PTS)
        total = jnp.sum(values * values, axis=0, keepdims=True)
        return jnp.where(lane == e, jnp.sum(total, axis=1, keepdims=True), carry)

    def sum_copy(stage, step):
        return pltpu.make_async_remote_copy(
            sum_mine.at[stage], sum_all.at[stage, stage_me[stage]],
            sum_send.at[stage], sum_recv.at[stage],
            device_id=stage_peer(stage, step)[1], device_id_type=MESH,
        )

    def sum_rest(stage, sem):
        return whole(sum_all.at[stage, pl.ds(0, stage_size[stage] - 1)], sem.at[stage])

    def sum_start(stage):
        for step in range(1, stage_size[stage]):
            sum_copy(stage, step).start()
        sum_all[stage, stage_me[stage]] = sum_mine[stage]

    def sum_end(stage):
        sum_rest(stage, sum_recv).wait_recv()
        total = sum_all[stage, 0]
        for k in range(1, stage_size[stage]):
            total = total + sum_all[stage, k]
        sum_mine[stage + 1] = total

    pl.semaphore_wait(barrier, len(met) + len(solvers) * (at_0 + 2 * at_1 + at_2))
    for copy in halo_copies(0):
        copy.start()
    state_loads[1].wait()
    for load in loads:
        load.start()
    for k in range(PIECES):
        inverse_load(k).start()
    sum_mine[0] = lax.fori_loop(0, MEMBERS, squares, jnp.zeros((1, PTS), F32))
    sum_start(0)

    def pack_and_send(step, carry):
        for k in range(STEP):
            pack(step * STEP + k)
        for copy in halo_copies(step):
            copy.start()
        return carry

    lax.fori_loop(1, STEPS, pack_and_send, 0)

    for load in loads:
        load.wait()

    def split_inverse(m, carry):
        high, low = split(inverse[m])
        inv_high[m] = high
        inv_low[m] = low
        return carry


    coupling_0 = jnp.where(low_half, TIME_STEP * CORIOLIS, TIME_STEP)
    coupling_1 = jnp.where(low_half, -TIME_STEP * CORIOLIS, -TIME_STEP * STRATIFICATION)
    coefficient = me * LOCAL + lax.rem(lane, LOCAL)
    interior = coefficient < 4 * LOCAL - 2

    def mode_copies(step):
        moved = lax.div(step + leaving, GROUPS)
        target = step + moved * FOREIGN
        rows = pl.ds(step * (STEP * BLOCK), STEP * BLOCK)
        target_rows = pl.ds(target * (STEP * BLOCK), STEP * BLOCK)
        return [
            pltpu.make_async_remote_copy(
                out_modes.at[q, rows], in_modes.at[me, target_rows],
                mode_send.at[0], mode_recv.at[target],
                device_id=at_plane(solvers[q], z + moved * (1 - 2 * upper)), device_id_type=MESH,
            )
            for q in range(4)
        ]

    def project_member(e):
        centre = state[e]
        rim_left, rim_right = rims[0, e], rims[1, e]
        top = jnp.where(low_half, rim_right, rim_left)
        low = pltpu.roll(jnp.where(low_half, rim_left, rim_right), LOCAL, 2)
        rim = jnp.concatenate([top, low], axis=1)
        segment = jnp.concatenate(
            [centre.reshape(FIELDS * LOCAL, PTS), rim.reshape(FIELDS * LOCAL, PTS)], axis=1
        )
        high, low = split(segment)
        first = dot_t(project[...], high)
        second = dot_t(project[: 2 * MODES], low)
        both = first[: 2 * MODES] + (first[2 * MODES :] + second)
        a_0, a_1 = both[:MODES, :PTS], both[:MODES, PTS:]
        b_0, b_1 = both[MODES:, :PTS], both[MODES:, PTS:]
        rhs_0 = jnp.where(interior, a_0 + coupling_0 * b_1, 0.0)
        rhs_1 = jnp.where(interior, a_1 + coupling_1 * b_0, 0.0)
        for q in range(4):
            modes = slice(q * QUARTER, (q + 1) * QUARTER)
            base = pl.multiple_of(e * BLOCK, BLOCK)
            out_modes[q, pl.ds(base, QUARTER), :] = rhs_0[modes]
            out_modes[q, pl.ds(base + QUARTER, QUARTER), :] = rhs_1[modes]

    def project_step(step, carry):
        whole(rims.at[:, pl.ds(step * STEP, STEP)], halo_recv.at[step]).wait_recv()
        for k in range(STEP):
            project_member(step * STEP + k)
        for copy in mode_copies(step):
            copy.start()

        @pl.when(step < PIECES)
        def _():
            inverse_load(step).wait()
            lax.fori_loop(step * PIECE, (step + 1) * PIECE, split_inverse, 0)

        @pl.when(step == 2)
        def _():
            sum_end(0)
            sum_start(1)

        @pl.when(step == 4)
        def _():
            sum_end(1)
            sum_start(2)

        return carry

    lax.fori_loop(0, STEPS, project_step, 0)

    def back_to(slot, t):
        return at_plane(solvers[t], z + lax.div(slot, GROUPS) * (2 * upper - 1))

    def coef_copies(slot):
        target = slot - lax.div(slot, GROUPS) * FOREIGN
        rows = pl.ds(slot * (STEP * BLOCK), STEP * BLOCK)
        target_rows = pl.ds(target * (STEP * BLOCK), STEP * BLOCK)
        return [
            pltpu.make_async_remote_copy(
                out_coefs.at[t, rows], in_coefs.at[me, target_rows],
                coef_send.at[0], coef_recv.at[target],
                device_id=back_to(slot, t), device_id_type=MESH,
            )
            for t in range(4)
        ]

    def wall_copies(slot):
        group = slot - lax.div(slot, GROUPS) * FOREIGN
        return [
            pltpu.make_async_remote_copy(
                wall_out.at[slot], wall_in.at[me, group],
                coef_send.at[1], wall_recv.at[group],
                device_id=back_to(slot, t), device_id_type=MESH,
            )
            for t in range(4)
        ]

    def wall_sums(slot):
        rows = pl.ds(slot * (GROUP * BLOCK), GROUP * BLOCK)
        blocks = jnp.concatenate([out_coefs[t, rows, :] for t in range(4)], axis=1)
        high, low = split(blocks)
        first = dot_t(weights[...], high)
        second = dot_t(weights[:16], low)
        wall_out[slot] = (first[:16] + (first[16:] + second))[:2]

    def solved_here(slot):
        own = (slot < GROUPS) & (slot < GROUPS - leaving)
        return own | ((slot >= GROUPS) & (slot >= SLOTS - coming))

    def turn(a):
        return pltpu.roll(a, LOCAL, 1)

    def solve_mode(base, m):
        rows = pl.ds(base + m, 2 * GROUP, stride=QUARTER)
        parts = [in_modes[s, rows, :] for s in range(4)]
        even, odd = [], []
        for s in (0, 2):
            first, second = parts[s], parts[s + 1]
            even.append(jnp.where(low_half, first, turn(second)))
            odd.append(jnp.where(low_half, turn(first), second))
        values = jnp.concatenate(
            [jnp.concatenate(even, axis=1), jnp.concatenate(odd, axis=1)], axis=0
        )
        high, low = split(values)
        count = 4 * GROUP
        first = dot_t(jnp.concatenate([high, low], axis=0), inv_high[m])
        second = dot_t(high, inv_low[m])
        solved = first[:count] + (first[count:] + second)
        even, odd = solved[: 2 * GROUP], solved[2 * GROUP :]
        for k in range(2):
            lanes = slice(k * PTS, (k + 1) * PTS)
            out_coefs[2 * k, rows, :] = jnp.where(low_half, even[:, lanes], turn(odd[:, lanes]))
            out_coefs[2 * k + 1, rows, :] = jnp.where(low_half, turn(even[:, lanes]), odd[:, lanes])

    def solve_group(group):
        rows = pl.ds(group * (GROUP * BLOCK), GROUP * BLOCK)
        whole(in_modes.at[:, rows], mode_recv.at[group]).wait_recv()
        base = group * (GROUP * BLOCK)

        def some_modes(k, carry):
            for u in range(UNROLL):
                solve_mode(base, k * UNROLL + u)
            return carry

        lax.fori_loop(0, QUARTER // UNROLL, some_modes, 0)
        for copy in coef_copies(group):
            copy.start()
        wall_sums(group)
        for copy in wall_copies(group):
            copy.start()

    def solve_slot(turn, carry):
        def from_turn(n):
            return lax.div(turn + SLOTS - n, SLOTS)

        slot = turn + 3 * from_turn(3) - 4 * from_turn(4) + 3 * from_turn(5) - 5 * from_turn(7)

        @pl.when(solved_here(slot))
        def _():
            solve_group(slot)

        return carry

    lax.fori_loop(0, SLOTS, solve_slot, 0)

    whole(sides, halo_send.at[0]).wait_send()
    whole(out_modes, mode_send.at[0]).wait_send()
    for stage in range(3):
        sum_rest(stage, sum_send).wait_send()

    grid = float(FIELDS * 4 * LOCAL * PTS * count)

    sum_end(2)

    def back_member(e):
        base = pl.multiple_of(e * BLOCK, BLOCK)
        turned = []
        for col in range(2):
            block = jnp.concatenate(
                [in_coefs[q, pl.ds(base + col * QUARTER, QUARTER), :] for q in range(4)], axis=0
            )
            turned.append(block.T)
        high, low = split(jnp.concatenate(turned, axis=0))
        values = dot(jnp.concatenate([high, low], axis=1), back[: 2 * MODES])
        values = values + dot(high, back[2 * MODES : 3 * MODES])
        total = jnp.sum(jnp.where(lane == e, sum_mine[3], 0.0), axis=1, keepdims=True)
        values = values * lax.rsqrt(total / grid + EPSILON)
        out_ref[e] = values.reshape(FIELDS, LOCAL, PTS)

    row = lax.broadcasted_iota(jnp.int32, (4 * GROUP, SPAN), 0)
    lanes = lax.broadcasted_iota(jnp.int32, (4 * GROUP, SPAN), 1)
    own = lax.div(lanes, QUARTER) == 2 * lax.div(row, 4) + lax.rem(row, 2)
    upper_wall = lax.rem(lax.div(row, 2), 2) == 0

    def wall_group(group):
        whole(wall_in.at[:, group], wall_recv.at[group]).wait_recv()
        parts = []
        for q in range(4):
            both = wall_in[q, group]
            parts.append(jnp.where(own, jnp.where(upper_wall, both[:1], both[1:]), 0.0))
        high, low = split(jnp.concatenate(parts, axis=1))
        table = back[3 * MODES : 3 * MODES + 4 * SPAN]
        first = dot(jnp.concatenate([high, low], axis=0), table)
        count = 4 * GROUP
        values = first[:count] + (first[count:] + dot(high, back[3 * MODES + 4 * SPAN :]))
        member = group * GROUP + lax.div(row[:, :PTS], 4)
        total = jnp.sum(jnp.where(lane == member, sum_mine[3], 0.0), axis=1, keepdims=True)
        values = values * lax.rsqrt(total / grid + EPSILON)
        for e in range(GROUP):
            for w in range(2):
                wall_ref[group * GROUP + e, w] = values[4 * e + 2 * w : 4 * e + 2 * w + 2]

    def back_step(step, carry):
        rows = pl.ds(step * (STEP * BLOCK), STEP * BLOCK)
        whole(in_coefs.at[:, rows], coef_recv.at[step]).wait_recv()
        for k in range(STEP):
            back_member(step * STEP + k)

        wall_group(step)
        return carry

    lax.fori_loop(0, STEPS, back_step, 0)

    for held, here_now in (
        (GROUPS - MOVED[0], depth == 0), (GROUPS - MOVED[1] + MOVED[0], depth == 1),
        (GROUPS + MOVED[1], depth == 2), (GROUPS, depth > 2),
    ):
        @pl.when(here_now)
        def _():
            whole(out_coefs.at[:, pl.ds(0, held * GROUP * BLOCK)], coef_send.at[0]).wait_send()
            whole(wall_in.at[:, pl.ds(0, held)], coef_send.at[1]).wait_send()


def per_device(sizes, state, inverse):
    both, back = window_tables(PTS + 2 * HALO, HALO, PTS, MODES)
    project = jnp.asarray(np.concatenate(split_table(both), axis=0))
    high, low = split_table(back)

    def tiled(table):
        quarters = table.reshape(4, QUARTER, PTS)
        return np.concatenate([q for part in quarters for q in [part] * (2 * GROUP)], axis=0)

    back = jnp.asarray(np.concatenate([high, high, low, tiled(high), tiled(low)], axis=0))
    k = np.arange(4 * LOCAL, dtype=np.float64)
    curvature = k * k / (4 * LOCAL) ** 2
    walls = np.zeros((16, 4, 2, LOCAL))
    walls[0, :, 0] = curvature.reshape(4, LOCAL)
    walls[1, :, 0] = np.where(k % 2 == 0, -curvature, curvature).reshape(4, LOCAL)
    weights = jnp.asarray(np.concatenate(split_table(walls.reshape(16, 8 * LOCAL)), axis=0))
    exchange = (4, MEMBERS * BLOCK, PTS)
    larger = (4, SLOTS * GROUP * BLOCK + QUARTER, PTS)
    rim = (2, MEMBERS, FIELDS, 32, PTS)
    vmem = pltpu.VMEM
    dma = pltpu.SemaphoreType.DMA
    updated, wall = pl.pallas_call(
        functools.partial(kernel, sizes),
        out_shape=(
            pltpu.VMEM(state.shape, F32),
            pltpu.VMEM((MEMBERS, 2, 2, PTS), F32),
        ),
        in_specs=[pl.BlockSpec(memory_space=pl.ANY)] * 5,
        out_specs=(
            pl.BlockSpec(memory_space=pltpu.VMEM),
            pl.BlockSpec(memory_space=pltpu.VMEM),
        ),
        scratch_shapes=[
            vmem(state.shape, F32),
            vmem(inverse.shape, F32),
            vmem(inverse.shape, BF16),
            vmem(inverse.shape, BF16),
            vmem(project.shape, BF16),
            vmem(back.shape, BF16),
            vmem(weights.shape, BF16),
            *[vmem(rim, F32)] * 2,
            vmem(exchange, F32),
            vmem(larger, F32),
            vmem(larger, F32),
            vmem(exchange, F32),
            vmem((4, 1, PTS), F32),
            vmem((3, 8, 1, PTS), F32),
            vmem((SLOTS, 2, SPAN), F32),
            vmem((4, SLOTS, 2, SPAN), F32),
            dma((9,)),
            dma((1,)),
            dma((STEPS,)),
            dma((1,)),
            dma((SLOTS,)),
            dma((2,)),
            dma((STEPS,)),
            dma((3,)),
            dma((3,)),
            dma((GROUPS,)),
        ],
        compiler_params=pltpu.CompilerParams(
            collective_id=0, has_side_effects=True, vmem_limit_bytes=56 * 1024 * 1024
        ),
        name="step",
    )(state, inverse, project, back, weights)
    return updated, wall


def solution(mesh):
    torus = Mesh(mesh.devices.reshape(4, 2, 8, 2, 2), AXES)
    return jax.shard_map(
        functools.partial(per_device, (4, 2, 8)),
        mesh=torus,
        in_specs=(P(None, None, GY, GX), P(GY, None, None)),
        out_specs=(P(None, None, GY, GX), P(None, None, None, GX)),
        check_vma=False,
    )
```
